128 devices in a mesh: chan: 4 (over x_lo, core), slab: 32 (over y, z, x_hi).
Axes of the slice: x: 4 (x_hi: 2, x_lo: 2; x = x_hi * 2 + x_lo), y: 4, z: 4, core: 2. Of those that a mesh axis runs over, the one named last changes fastest.
Arguments:
- beam_images: float32 [64, 2048, 4096], P('chan', 'slab'), may hold values from -24 to 24
- chan_weights: int32 [64], P('chan'), may hold values from 1 to 8
- freq_offsets: float32 [64], P('chan'), may hold values from -1 to 1
- half_widths: int32 [5], replicated, may hold values from 16 to 32, as said below
Outputs:
- smoothed: float32 [5, 2048, 4096], P(None, 'slab', 'chan')
The draws below stay inside these ranges and needn't reach their ends.
Inputs may be any that keep to these rules, and one draw needn't show every extreme that they name: `half_widths`: each half-width is at least 16 and at most 32; at least one equals 32.
All inputs are finite; a program needn't handle non-finite values.
Results may differ from the reference program's by a relative error of at most 0.00008.
Values sent between devices are 32-bit elements; how exact they have to be, the bound alone decides.
A program may use at most 128 MiB of HBM per device.

```python
import jax
import jax.numpy as jnp
from jax import lax

NCHAN = 64
NCOLS = 4096
MOMENTS = 5
HW_MAX = 32
NROWS = 2048


def draw_half_widths(key, part):
    first_key, second_key = jax.random.split(jax.random.fold_in(key, 17))
    values = jax.random.randint(first_key, (MOMENTS,), HW_MAX // 2, HW_MAX + 1)
    chosen = jax.random.randint(second_key, (), 0, MOMENTS)
    return jnp.where(jnp.arange(MOMENTS) == chosen, HW_MAX, values).astype(jnp.int32)


def with_ends(array, stream_key, low, largest):
    dims = array.shape
    spot = [jax.random.randint(jax.random.fold_in(stream_key, axis), (), 0, dims[axis]) for axis in range(len(dims))]
    array = array.at[tuple(spot)].set(low)
    longest = dims.index(max(dims))
    spot[longest] = (spot[longest] + 1) % dims[longest]
    return array.at[tuple(spot)].set(largest)


def block_scale(stream_key, extent, cuts, smallest, largest):
    gain, own = 1.0, jax.random.fold_in(stream_key, 6)
    for axis_at, blocks in cuts:
        heights = jnp.exp(jax.random.uniform(jax.random.fold_in(own, axis_at), (blocks,), jnp.float32, smallest / len(cuts), largest / len(cuts)))
        gain = gain * jnp.repeat(heights, extent[axis_at] // blocks).reshape([-1 if axis == axis_at else 1 for axis in range(len(extent))])
    return gain


def gaussian(own_key, extent, deviation, bound, pieces=(), dtype=jnp.bfloat16):
    result = jax.random.normal(own_key, extent, jnp.float32) * deviation
    if len(pieces) > 0:
        result = block_scale(own_key, extent, pieces, -0.22, 0.18) * result
    return jnp.clip(result, min=-bound, max=bound).astype(dtype)


def setup_inputs(seed: int = 0) -> dict:
    streams_of = jax.random.split(jax.random.key(seed), 5)
    return {
        "beam_images": gaussian(streams_of[0], (NCHAN, NROWS, NCOLS), 4.0, 24.0, ((0, 4), (1, 32)), jnp.float32),
        "chan_weights": with_ends(jax.random.randint(streams_of[1], (NCHAN,), 1, 9), jax.random.fold_in(streams_of[1], 1), 1, 8).astype(jnp.int32),
        "freq_offsets": jnp.clip(jax.random.uniform(streams_of[2], (NCHAN,), jnp.float32, -1.0, 1.0) * block_scale(streams_of[2], (NCHAN,), ((0, 4),), -0.4, 0.0), -1.0, 1.0),
        "half_widths": draw_half_widths(jax.random.fold_in(streams_of[4], 71), 0),
    }


def window_sum(values, reach, along):
    length = values.shape[along]
    widths = [(0, 0)] * values.ndim
    widths[along] = (HW_MAX + 1, HW_MAX)
    padded = jnp.pad(values, widths)
    running = jnp.cumsum(padded, axis=along)
    upper = lax.dynamic_slice_in_dim(running, (HW_MAX + 1 + reach).astype(jnp.int32), length, along)
    lower = lax.dynamic_slice_in_dim(running, (HW_MAX - reach).astype(jnp.int32), length, along)
    return upper - lower


def reference(beam_images, chan_weights, freq_offsets, half_widths):
    weight_floats = chan_weights.astype(jnp.float32)
    weight_total = jnp.sum(weight_floats)
    powers = jnp.stack([freq_offsets ** power for power in range(MOMENTS)])
    coefficients = powers * weight_floats[None, :] / weight_total
    flat = beam_images.reshape(NCHAN, NROWS * NCOLS)
    moments = jnp.dot(coefficients, flat, precision=lax.Precision.HIGHEST, preferred_element_type=jnp.float32)
    moments = moments.reshape(MOMENTS, NROWS, NCOLS)
    results = []
    for power in range(MOMENTS):
        reach = half_widths[power]
        summed = window_sum(window_sum(moments[power], reach, 0), reach, 1)
        results.append(summed / (2 * reach + 1).astype(jnp.float32))
    return jnp.stack(results)
```

```python
import functools

import jax
import jax.numpy as jnp
from jax import lax
from jax.experimental import pallas as pl
from jax.experimental.pallas import tpu as pltpu
from jax.sharding import PartitionSpec as P

MESH = pl.DeviceIdType.MESH
MOMENTS = 5
HW = 32
LANES = 128
F32 = jnp.float32
BF16 = jnp.bfloat16


def halves(value):
    high = value.astype(BF16)
    low = (value - high.astype(F32)).astype(BF16)
    return high, low


def kernel(
    slabs, tiles, chans,
    beam, weights, offsets, reach, out,
    pix, part, got, from_same_far, from_same_own, from_direct, to_other, from_other,
    to_direct, from_rows, rows, done, row_band, col_band, coef, w_mine, w_got,
    pix_sem, core_send, core_recv, far_send, far_recv, own_send, own_recv,
    dir_send, dir_recv, oth_send, oth_recv, row_send, row_recv,
    edge_send, edge_recv, w_send, w_recv, out_sem,
):
    chan = lax.axis_index("chan")
    slab = lax.axis_index("slab")
    odd = slab % 2
    partner = (chan + 2) % 4
    other_core = chan + 1 - 2 * (chan % 2)
    far_core = 3 - chan
    same_slab = slab + 1 - 2 * odd
    other_slab = (slab + slabs - 1 + 2 * odd) % slabs
    half_same = 1 - odd
    half_other = odd
    to_core = (other_core, slab)
    to_partner = (partner, slab)
    to_far_core = (far_core, slab)
    to_wrap = (partner, same_slab)
    to_wrap_other = (partner, other_slab)

    def tile_of(order):
        return (tiles - order) % tiles

    def pixels(t, slot):
        quarter = (other_core, far_core, chan, partner)[slot]
        start = pl.multiple_of((quarter * tiles + t) * LANES, LANES)
        return pltpu.make_async_copy(beam.at[:, :, pl.ds(start, LANES)], pix.at[t, slot], pix_sem.at[t, slot])

    def remote(src, dst, send, recv, where):
        return pltpu.make_async_remote_copy(
            src_ref=src, dst_ref=dst, send_sem=send, recv_sem=recv, device_id=where, device_id_type=MESH
        )

    def core_copy(t):
        return remote(part.at[t, pl.ds(0, 2)], got.at[t], core_send.at[t], core_recv.at[t], to_core)

    def far_copy(t):
        return remote(part.at[t, 2, half_same], from_same_far.at[t], far_send.at[t], far_recv.at[t], to_wrap)

    def own_copy(t):
        return remote(part.at[t, 3, half_same], from_same_own.at[t], own_send.at[t], own_recv.at[t], to_wrap)

    def direct_copy(t):
        return remote(part.at[t, 2, half_other], from_direct.at[t], dir_send.at[t], dir_recv.at[t], to_partner)

    def other_copy(t):
        return remote(to_other.at[t], from_other.at[t], oth_send.at[t], oth_recv.at[t], to_wrap_other)

    def row_copy(t):
        return remote(to_direct.at[t], from_rows.at[t], row_send.at[t], row_recv.at[t], to_partner)

    def left_edge():
        return remote(rows.at[1], rows.at[tiles + 1], edge_send.at[0], edge_recv.at[1], ((chan + 3) % 4, slab))

    def right_edge():
        return remote(rows.at[tiles], rows.at[0], edge_send.at[1], edge_recv.at[0], ((chan + 1) % 4, slab))

    def weight_copy(i):
        return remote(w_mine, w_got.at[i], w_send.at[i], w_recv.at[i], (to_core, to_partner, to_far_core)[i])

    def result(t):
        start = pl.multiple_of(t * LANES, LANES)
        return pltpu.make_async_copy(done.at[t], out.at[:, :, pl.ds(start, LANES)], out_sem.at[t])

    def each(first, last, body):
        def step(order, carry):
            body(tile_of(order))
            return carry

        lax.fori_loop(first, last, step, 0)

    def fetch(t):
        for slot in range(4):
            pixels(t, slot).start()

    def moments(t, first):
        for slot in (first, first + 1):
            pixels(t, slot).wait()

        def block(index, carry):
            slot = first + index // 2
            half = index % 2
            start = pl.multiple_of(half * 32, 32)
            totals = [None] * MOMENTS
            for c in range(chans):
                x = pix[t, slot, c, pl.ds(start, 32), :]
                for k in range(MOMENTS):
                    term = coef[k * chans + c] * x
                    totals[k] = term if c == 0 else totals[k] + term
            for k in range(MOMENTS):
                part[t, slot, half, k] = totals[k]
            return carry

        lax.fori_loop(0, 4, block, 0)

    def make(t):
        moments(t, 0)
        core_copy(t).start()
        moments(t, 2)

    def join(t):
        core_copy(t).wait_recv()
        for side in range(2):
            for half in range(2):
                for k in range(MOMENTS):
                    part[t, 2 + side, half, k] = part[t, 2 + side, half, k] + got[t, side, half, k]
        far_copy(t).start()
        direct_copy(t).start()

    def row_sum(k, pieces):
        high, low = halves(jnp.concatenate(pieces, axis=0))
        band = row_band[k]
        return jnp.dot(band, high, preferred_element_type=F32) + jnp.dot(band, low, preferred_element_type=F32)

    def relay(t):
        direct_copy(t).wait_recv()
        to_other[t] = part[t, 3, half_other] + from_direct[t]
        other_copy(t).start()

    def give_rows(t):
        far_copy(t).wait_recv()
        blank = jnp.zeros((32, LANES), F32)
        for k in range(MOMENTS):
            to_direct[t, k] = row_sum(k, [part[t, 3, 0, k], part[t, 3, 1, k], from_same_far[t, k], blank])
        row_copy(t).start()

    def take_rows(t):
        own_copy(t).wait_recv()
        other_copy(t).wait_recv()
        sums = [
            row_sum(k, [part[t, 2, 0, k], part[t, 2, 1, k], from_same_own[t, k], from_other[t, k]])
            for k in range(MOMENTS)
        ]
        row_copy(t).wait_recv()
        for k in range(MOMENTS):
            rows[t + 1, k] = sums[k] + from_rows[t, k]

    def finish(t, scales):
        for k in range(MOMENTS):
            wide = jnp.concatenate([rows[t, k], rows[t + 1, k], rows[t + 2, k]], axis=1)
            high, low = halves(wide)
            band = col_band[k]
            total = jnp.dot(high, band, preferred_element_type=F32) + jnp.dot(low, band, preferred_element_type=F32)
            done[t, k] = (total.reshape(8, 8, LANES) * scales[k][None]).reshape(64, LANES)
        result(t).start()

    each(0, tiles, fetch)
    barrier = pltpu.get_barrier_semaphore()
    friends = (to_core, to_partner, to_far_core, to_wrap, to_wrap_other)
    for friend in friends:
        pl.semaphore_signal(barrier, inc=1, device_id=friend, device_id_type=MESH)

    weight_sum = F32(0)
    for c in range(chans):
        weight = weights[c].astype(F32)
        weight_sum = weight_sum + weight
        offset = offsets[c]
        value = weight
        for k in range(MOMENTS):
            coef[k * chans + c] = value
            value = value * offset
    w_mine[...] = jnp.full((8, LANES), weight_sum, F32)

    at_edge = jnp.logical_or(slab == 0, slab == slabs - 1)
    near = lax.broadcasted_iota(jnp.int32, (64, LANES), 0)
    lane = lax.broadcasted_iota(jnp.int32, (64, LANES), 1)
    same_shift = jnp.where(odd == 1, -96, 0)
    other_shift = jnp.where(at_edge, 1000, jnp.where(odd == 1, -32, -128))
    place = lane + jnp.where(lane < 64, 0, jnp.where(lane < 96, same_shift, other_shift))
    row_gap = jnp.abs(place - near)
    col_gap = jnp.abs(
        lax.broadcasted_iota(jnp.int32, (3 * LANES, LANES), 0) - LANES
        - lax.broadcasted_iota(jnp.int32, (3 * LANES, LANES), 1)
    )
    for k in range(MOMENTS):
        row_band[k] = jnp.where(row_gap <= reach[k], 1.0, 0.0).astype(BF16)
        col_band[k] = jnp.where(col_gap <= reach[k], 1.0, 0.0).astype(BF16)

    @pl.when(chan == 0)
    def _():
        rows[0] = jnp.zeros((MOMENTS, 64, LANES), F32)

    @pl.when(chan == 3)
    def _():
        rows[tiles + 1] = jnp.zeros((MOMENTS, 64, LANES), F32)

    pl.semaphore_wait(barrier, len(friends))
    make(tile_of(0))

    def making(order, carry):
        make(tile_of(order))
        join(tile_of(order - 1))
        return carry

    early = 2
    lax.fori_loop(1, early + 1, making, 0)
    each(0, early, lambda t: own_copy(t).start())
    for i in range(3):
        weight_copy(i).start()
    lax.fori_loop(early + 1, tiles, making, 0)
    join(tile_of(tiles - 1))

    def passing(t):
        relay(t)
        own_copy(t).start()
        give_rows(t)

    def passing_first(t):
        relay(t)
        give_rows(t)

    middle = max(early, (5 * tiles) // 8)
    each(0, early, passing_first)
    each(early, middle, passing)
    each(0, early, take_rows)

    @pl.when(chan > 0)
    def _():
        left_edge().start()

    @pl.when(chan < 3)
    def _():
        right_edge().start()

    each(middle, tiles, passing)

    for i in range(3):
        weight_copy(i).wait()
    total = w_mine[...] + w_got[0] + w_got[1] + w_got[2]
    scales = [1.0 / (total * (2 * reach[k] + 1).astype(F32)) for k in range(MOMENTS)]

    @pl.when(chan < 3)
    def _():
        left_edge().wait_recv()

    def finishing(order, carry):
        t = tile_of(order)
        take_rows(t)
        finish(t + 1, scales)
        return carry

    lax.fori_loop(early, tiles, finishing, 0)

    @pl.when(chan > 0)
    def _():
        right_edge().wait_recv()

    finish(1, scales)
    finish(0, scales)

    def drain(t):
        for copy in (core_copy, far_copy, own_copy, direct_copy, other_copy, row_copy):
            copy(t).wait_send()
        result(t).wait()

    each(0, tiles, drain)

    @pl.when(chan > 0)
    def _():
        left_edge().wait_send()

    @pl.when(chan < 3)
    def _():
        right_edge().wait_send()


def solution(mesh):
    slabs = mesh.shape["slab"]

    def body(beam, weights, offsets, reach):
        chans, height, width = beam.shape
        tiles = width // (4 * LANES)
        halo = (tiles, MOMENTS, 32, LANES)
        full = (MOMENTS, 64, LANES)
        dma = pltpu.SemaphoreType.DMA
        smem = pl.BlockSpec(memory_space=pltpu.SMEM)
        return pl.pallas_call(
            functools.partial(kernel, slabs, tiles, chans),
            out_shape=jax.ShapeDtypeStruct((MOMENTS, height, width // 4), F32),
            in_specs=[pl.BlockSpec(memory_space=pl.ANY), smem, smem, smem],
            out_specs=pl.BlockSpec(memory_space=pl.ANY),
            scratch_shapes=[
                pltpu.VMEM((tiles, 4, chans, 64, LANES), F32),
                pltpu.VMEM((tiles, 4, 2, MOMENTS, 32, LANES), F32),
                pltpu.VMEM((tiles, 2, 2, MOMENTS, 32, LANES), F32),
                pltpu.VMEM(halo, F32),
                pltpu.VMEM(halo, F32),
                pltpu.VMEM(halo, F32),
                pltpu.VMEM(halo, F32),
                pltpu.VMEM(halo, F32),
                pltpu.VMEM((tiles, *full), F32),
                pltpu.VMEM((tiles, *full), F32),
                pltpu.VMEM((tiles + 2, *full), F32),
                pltpu.VMEM((tiles, *full), F32),
                pltpu.VMEM((MOMENTS, 64, LANES), BF16),
                pltpu.VMEM((MOMENTS, 3 * LANES, LANES), BF16),
                pltpu.SMEM((MOMENTS * chans,), F32),
                pltpu.VMEM((8, LANES), F32),
                pltpu.VMEM((3, 8, LANES), F32),
                dma((tiles, 4)),
                dma((tiles,)), dma((tiles,)),
                dma((tiles,)), dma((tiles,)),
                dma((tiles,)), dma((tiles,)),
                dma((tiles,)), dma((tiles,)),
                dma((tiles,)), dma((tiles,)),
                dma((tiles,)), dma((tiles,)),
                dma((2,)), dma((2,)),
                dma((3,)), dma((3,)),
                dma((tiles,)),
            ],
            compiler_params=pltpu.CompilerParams(
                collective_id=0, has_side_effects=True, vmem_limit_bytes=60 * 1024 * 1024
            ),
        )(beam, weights, offsets, reach)

    placed = (P("chan", "slab", None), P("chan"), P("chan"), P())
    return jax.shard_map(
        body, mesh=mesh, in_specs=placed, out_specs=P(None, "slab", "chan"), check_vma=False
    )
```

```python
import functools

import jax
import jax.numpy as jnp
from jax import lax
from jax.experimental import pallas as pl
from jax.experimental.pallas import tpu as pltpu
from jax.sharding import PartitionSpec as P

MESH = pl.DeviceIdType.MESH
MOMENTS = 5
HW = 32
LANES = 128
F32 = jnp.float32
BF16 = jnp.bfloat16


def halves(value):
    high = value.astype(BF16)
    low = (value - high.astype(F32)).astype(BF16)
    return high, low


def kernel(
    slabs, tiles, chans,
    beam, weights, offsets, reach, out,
    pix, part, got, from_same_far, from_same_own, from_direct, to_other, from_other,
    to_direct, from_rows, rows, row_band, col_band, coef, w_mine, w_pair, w_got,
    pix_sem, core_send, core_recv, far_send, far_recv, own_send, own_recv,
    dir_send, dir_recv, oth_send, oth_recv, row_send, row_recv,
    edge_send, edge_recv, w_send, w_recv, ready, other_ready,
):
    chan = lax.axis_index("chan")
    slab = lax.axis_index("slab")
    odd = slab % 2
    partner = (chan + 2) % 4
    other_core = chan + 1 - 2 * (chan % 2)
    far_core = 3 - chan
    same_slab = slab + 1 - 2 * odd
    other_slab = (slab + slabs - 1 + 2 * odd) % slabs
    half_same = 1 - odd
    half_other = odd
    to_core = (other_core, slab)
    to_partner = (partner, slab)
    to_far_core = (far_core, slab)
    caller = jnp.logical_or(chan == 0, chan == 3)
    callee = jnp.logical_not(caller)
    at_edge = jnp.logical_or(slab == 0, slab == slabs - 1)
    inside = jnp.logical_not(at_edge)
    to_wrap = (partner, same_slab)
    to_wrap_other = (partner, other_slab)

    def tile_of(order):
        return (tiles - order) % tiles

    def pixels(t, slot):
        quarter = (other_core, far_core, chan, partner)[slot]
        start = pl.multiple_of((quarter * tiles + t) * LANES, LANES)
        return pltpu.make_async_copy(beam.at[:, :, pl.ds(start, LANES)], pix.at[t, slot], pix_sem.at[t, slot])

    def remote(src, dst, send, recv, where):
        return pltpu.make_async_remote_copy(
            src_ref=src, dst_ref=dst, send_sem=send, recv_sem=recv, device_id=where, device_id_type=MESH
        )

    def core_copy(t):
        return remote(part.at[t, pl.ds(0, 2)], got.at[t], core_send.at[t], core_recv.at[t], to_core)

    def far_copy(t):
        return remote(part.at[t, 2, half_same], from_same_far.at[t], far_send.at[t], far_recv.at[t], to_wrap)

    def own_copy(t):
        return remote(part.at[t, 3, half_same], from_same_own.at[t], own_send.at[t], own_recv.at[t], to_wrap)

    def direct_copy(t):
        return remote(part.at[t, 2, half_other], from_direct.at[t], dir_send.at[t], dir_recv.at[t], to_partner)

    def other_copy(t):
        return remote(to_other.at[t], from_other.at[t], oth_send.at[t], oth_recv.at[t], to_wrap_other)

    def row_copy(t):
        return remote(to_direct.at[t], from_rows.at[t], row_send.at[t], row_recv.at[t], to_partner)

    def left_edge():
        return remote(rows.at[1], rows.at[tiles + 1], edge_send.at[0], edge_recv.at[1], ((chan + 3) % 4, slab))

    def right_edge():
        return remote(rows.at[tiles], rows.at[0], edge_send.at[1], edge_recv.at[0], ((chan + 1) % 4, slab))

    def weight_copy(i):
        return remote((w_mine, w_pair)[i], w_got.at[i], w_send.at[i], w_recv.at[i], (to_core, to_partner)[i])

    def each(first, last, body):
        def step(order, carry):
            body(tile_of(order))
            return carry

        lax.fori_loop(first, last, step, 0)

    def fetch(t):
        for slot in range(4):
            pixels(t, slot).start()

    def moments(t, first):
        for slot in (first, first + 1):
            pixels(t, slot).wait()

        def block(index, carry):
            slot = first + index // 2
            half = index % 2
            start = pl.multiple_of(half * 32, 32)
            totals = [None] * MOMENTS
            for c in range(chans):
                x = pix[t, slot, c, pl.ds(start, 32), :]
                for k in range(MOMENTS):
                    term = coef[k * chans + c] * x
                    totals[k] = term if c == 0 else totals[k] + term
            for k in range(MOMENTS):
                part[t, slot, half, k] = totals[k]
            return carry

        lax.fori_loop(0, 4, block, 0)

    def make_early(t):
        moments(t, 0)
        moments(t, 2)

    def make(t):
        moments(t, 0)
        core_copy(t).start()
        moments(t, 2)

    def join(t):
        core_copy(t).wait_recv()
        for side in range(2):
            for half in range(2):
                for k in range(MOMENTS):
                    part[t, 2 + side, half, k] = part[t, 2 + side, half, k] + got[t, side, half, k]
        far_copy(t).start()
        direct_copy(t).start()

    def row_sum(k, pieces):
        high, low = halves(jnp.concatenate(pieces, axis=0))
        band = row_band[k]
        return jnp.dot(band, high, preferred_element_type=F32) + jnp.dot(band, low, preferred_element_type=F32)

    def relay(t):
        direct_copy(t).wait_recv()
        to_other[t] = part[t, 3, half_other] + from_direct[t]

        @pl.when(inside)
        def _():
            other_copy(t).start()

    def give_rows(t):
        far_copy(t).wait_recv()
        blank = jnp.zeros((32, LANES), F32)
        for k in range(MOMENTS):
            to_direct[t, k] = row_sum(k, [part[t, 3, 0, k], part[t, 3, 1, k], from_same_far[t, k], blank])
        row_copy(t).start()

    def take_rows(t):
        own_copy(t).wait_recv()

        @pl.when(inside)
        def _():
            other_copy(t).wait_recv()

        sums = [
            row_sum(k, [part[t, 2, 0, k], part[t, 2, 1, k], from_same_own[t, k], from_other[t, k]])
            for k in range(MOMENTS)
        ]
        row_copy(t).wait_recv()
        for k in range(MOMENTS):
            rows[t + 1, k] = sums[k] + from_rows[t, k]

    def finish(t, scales):
        for k in range(MOMENTS):
            wide = jnp.concatenate([rows[t, k], rows[t + 1, k], rows[t + 2, k]], axis=1)
            high, low = halves(wide)
            band = col_band[k]
            total = jnp.dot(high, band, preferred_element_type=F32) + jnp.dot(low, band, preferred_element_type=F32)
            start = pl.multiple_of(t * LANES, LANES)
            out[k, :, pl.ds(start, LANES)] = (total.reshape(8, 8, LANES) * scales[k][None]).reshape(64, LANES)

    each(0, tiles, fetch)
    barrier = pltpu.get_barrier_semaphore()

    def call(semaphore, where):
        pl.semaphore_signal(semaphore, inc=1, device_id=where, device_id_type=MESH)

    @pl.when(caller)
    def _():
        for friend in (to_core, to_partner, to_wrap):
            call(barrier, friend)

    @pl.when(callee)
    def _():
        call(barrier, to_far_core)

    @pl.when(jnp.logical_and(callee, inside))
    def _():
        call(barrier, to_wrap_other)

    weight_sum = F32(0)
    for c in range(chans):
        weight = weights[c].astype(F32)
        weight_sum = weight_sum + weight
        offset = offsets[c]
        value = weight
        for k in range(MOMENTS):
            coef[k * chans + c] = value
            value = value * offset
    w_mine[...] = jnp.full((8, LANES), weight_sum, F32)

    @pl.when(chan == 0)
    def _():
        rows[0] = jnp.zeros((MOMENTS, 64, LANES), F32)

    @pl.when(chan == 3)
    def _():
        rows[tiles + 1] = jnp.zeros((MOMENTS, 64, LANES), F32)

    @pl.when(at_edge)
    def _():
        from_other[...] = jnp.zeros_like(from_other)

    early = 2
    each(0, early, make_early)

    @pl.when(callee)
    def _():
        pl.semaphore_wait(barrier, 4)
        for friend in (to_core, to_partner, to_wrap):
            call(ready, friend)
        each(0, early, lambda t: core_copy(t).start())

    near = lax.broadcasted_iota(jnp.int32, (64, LANES), 0)
    lane = lax.broadcasted_iota(jnp.int32, (64, LANES), 1)
    same_shift = jnp.where(odd == 1, -96, 0)
    other_shift = jnp.where(at_edge, 1000, jnp.where(odd == 1, -32, -128))
    place = lane + jnp.where(lane < 64, 0, jnp.where(lane < 96, same_shift, other_shift))
    row_gap = jnp.abs(place - near)
    col_gap = jnp.abs(
        lax.broadcasted_iota(jnp.int32, (3 * LANES, LANES), 0) - LANES
        - lax.broadcasted_iota(jnp.int32, (3 * LANES, LANES), 1)
    )
    for k in range(MOMENTS):
        row_band[k] = jnp.where(row_gap <= reach[k], 1.0, 0.0).astype(BF16)
        col_band[k] = jnp.where(col_gap <= reach[k], 1.0, 0.0).astype(BF16)


    @pl.when(caller)
    def _():
        pl.semaphore_wait(ready, 3)
        each(0, early, lambda t: core_copy(t).start())

    def making(order, carry):
        make(tile_of(order))
        join(tile_of(order - early))
        return carry

    weight_copy(0).start()
    lax.fori_loop(early, tiles, making, 0)
    each(tiles - early, tiles, join)
    weight_copy(0).wait_recv()
    w_pair[...] = w_mine[...] + w_got[0]

    @pl.when(jnp.logical_and(caller, inside))
    def _():
        pl.semaphore_wait(barrier, 1)
        call(other_ready, to_wrap_other)

    @pl.when(jnp.logical_and(callee, inside))
    def _():
        pl.semaphore_wait(other_ready, 1)

    def passing(t):
        relay(t)
        own_copy(t).start()
        give_rows(t)

    def relaying(t):
        relay(t)
        own_copy(t).start()

    middle = max(early, (5 * tiles) // 8)
    each(0, middle, passing)
    each(middle, tiles, relaying)
    weight_copy(1).start()
    each(0, early, take_rows)

    @pl.when(chan > 0)
    def _():
        left_edge().start()

    @pl.when(chan < 3)
    def _():
        right_edge().start()

    each(middle, tiles, give_rows)

    weight_copy(1).wait_recv()
    total = w_pair[...] + w_got[1]
    scales = [1.0 / (total * (2 * reach[k] + 1).astype(F32)) for k in range(MOMENTS)]

    @pl.when(chan < 3)
    def _():
        left_edge().wait_recv()

    def finishing(order, carry):
        t = tile_of(order)
        take_rows(t)
        finish(t + 1, scales)
        return carry

    lax.fori_loop(early, tiles, finishing, 0)

    @pl.when(chan > 0)
    def _():
        right_edge().wait_recv()

    finish(1, scales)
    finish(0, scales)

    def drain(t):
        for copy in (core_copy, far_copy, own_copy, direct_copy, row_copy):
            copy(t).wait_send()

        @pl.when(inside)
        def _():
            other_copy(t).wait_send()

    each(0, tiles, drain)
    for i in range(2):
        weight_copy(i).wait_send()

    @pl.when(chan > 0)
    def _():
        left_edge().wait_send()

    @pl.when(chan < 3)
    def _():
        right_edge().wait_send()


def solution(mesh):
    slabs = mesh.shape["slab"]

    def body(beam, weights, offsets, reach):
        chans, height, width = beam.shape
        tiles = width // (4 * LANES)
        halo = (tiles, MOMENTS, 32, LANES)
        full = (MOMENTS, 64, LANES)
        dma = pltpu.SemaphoreType.DMA
        smem = pl.BlockSpec(memory_space=pltpu.SMEM)
        return pl.pallas_call(
            functools.partial(kernel, slabs, tiles, chans),
            out_shape=pltpu.VMEM((MOMENTS, height, width // 4), F32),
            in_specs=[pl.BlockSpec(memory_space=pl.ANY), smem, smem, smem],
            out_specs=pl.BlockSpec(memory_space=pltpu.VMEM),
            scratch_shapes=[
                pltpu.VMEM((tiles, 4, chans, 64, LANES), F32),
                pltpu.VMEM((tiles, 4, 2, MOMENTS, 32, LANES), F32),
                pltpu.VMEM((tiles, 2, 2, MOMENTS, 32, LANES), F32),
                pltpu.VMEM(halo, F32),
                pltpu.VMEM(halo, F32),
                pltpu.VMEM(halo, F32),
                pltpu.VMEM(halo, F32),
                pltpu.VMEM(halo, F32),
                pltpu.VMEM((tiles, *full), F32),
                pltpu.VMEM((tiles, *full), F32),
                pltpu.VMEM((tiles + 2, *full), F32),
                pltpu.VMEM((MOMENTS, 64, LANES), BF16),
                pltpu.VMEM((MOMENTS, 3 * LANES, LANES), BF16),
                pltpu.SMEM((MOMENTS * chans,), F32),
                pltpu.VMEM((8, LANES), F32),
                pltpu.VMEM((8, LANES), F32),
                pltpu.VMEM((2, 8, LANES), F32),
                dma((tiles, 4)),
                dma((tiles,)), dma((tiles,)),
                dma((tiles,)), dma((tiles,)),
                dma((tiles,)), dma((tiles,)),
                dma((tiles,)), dma((tiles,)),
                dma((tiles,)), dma((tiles,)),
                dma((tiles,)), dma((tiles,)),
                dma((2,)), dma((2,)),
                dma((2,)), dma((2,)),
                pltpu.SemaphoreType.REGULAR, pltpu.SemaphoreType.REGULAR,
            ],
            compiler_params=pltpu.CompilerParams(
                collective_id=0, has_side_effects=True, vmem_limit_bytes=60 * 1024 * 1024
            ),
        )(beam, weights, offsets, reach)

    placed = (P("chan", "slab", None), P("chan"), P("chan"), P())
    return jax.shard_map(
        body, mesh=mesh, in_specs=placed, out_specs=P(None, "slab", "chan"), check_vma=False
    )
```

```python
import functools

import jax
import jax.numpy as jnp
from jax import lax
from jax.experimental import pallas as pl
from jax.experimental.pallas import tpu as pltpu
from jax.sharding import PartitionSpec as P

MESH = pl.DeviceIdType.MESH
MOMENTS = 5
HW = 32
LANES = 128
F32 = jnp.float32
BF16 = jnp.bfloat16


def halves(value):
    high = value.astype(BF16)
    low = (value - high.astype(F32)).astype(BF16)
    return high, low


def kernel(
    slabs, tiles, chans,
    beam, weights, offsets, reach, out,
    pix, part, got, from_same_far, from_same_own, from_direct, to_other, from_other,
    to_direct, from_rows, rows, row_band, col_band, coef, w_mine, w_pair, w_got, edge_mine, edge_got,
    pix_sem, core_send, core_recv, far_send, far_recv, own_send, own_recv,
    dir_send, dir_recv, oth_send, oth_recv, row_send, row_recv,
    edge_send, edge_recv, w_send, w_recv, ready, other_ready,
):
    chan = lax.axis_index("chan")
    slab = lax.axis_index("slab")
    odd = slab % 2
    partner = (chan + 2) % 4
    other_core = chan + 1 - 2 * (chan % 2)
    far_core = 3 - chan
    same_slab = slab + 1 - 2 * odd
    other_slab = (slab + slabs - 1 + 2 * odd) % slabs
    half_same = 1 - odd
    half_other = odd
    to_core = (other_core, slab)
    to_partner = (partner, slab)
    to_far_core = (far_core, slab)
    caller = jnp.logical_or(chan == 0, chan == 3)
    callee = jnp.logical_not(caller)
    at_edge = jnp.logical_or(slab == 0, slab == slabs - 1)
    inside = jnp.logical_not(at_edge)
    to_wrap = (partner, same_slab)
    to_wrap_other = (partner, other_slab)

    def tile_of(order):
        return (tiles - order) % tiles

    def pixels(t, slot):
        quarter = (other_core, far_core, chan, partner)[slot]
        start = pl.multiple_of((quarter * tiles + t) * LANES, LANES)
        return pltpu.make_async_copy(beam.at[:, :, pl.ds(start, LANES)], pix.at[t, slot], pix_sem.at[t, slot // 2])

    def pixels_wait(t, pair):
        two = pix.at[t, pl.ds(2 * pair, 2)]
        pltpu.make_async_copy(two, two, pix_sem.at[t, pair]).wait()

    def remote(src, dst, send, recv, where):
        return pltpu.make_async_remote_copy(
            src_ref=src, dst_ref=dst, send_sem=send, recv_sem=recv, device_id=where, device_id_type=MESH
        )

    def core_copy(t):
        return remote(part.at[t, pl.ds(0, 2)], got.at[t], core_send, core_recv.at[t], to_core)

    def far_copy(t):
        return remote(part.at[t, 2, half_same], from_same_far.at[t], far_send, far_recv.at[t], to_wrap)

    def own_copy(t):
        return remote(part.at[t, 3, half_same], from_same_own.at[t], own_send, own_recv.at[t], to_wrap)

    def direct_copy(t):
        return remote(part.at[t, 2, half_other], from_direct.at[t], dir_send, dir_recv.at[t], to_partner)

    def other_copy(t):
        return remote(to_other.at[t], from_other.at[t], oth_send, oth_recv.at[t], to_wrap_other)

    def row_copy(t):
        return remote(to_direct.at[t], from_rows.at[t], row_send, row_recv.at[t], to_partner)

    def left_edge():
        return remote(edge_mine.at[0], edge_got.at[1], edge_send.at[0], edge_recv.at[1], ((chan + 3) % 4, slab))

    def right_edge():
        return remote(edge_mine.at[1], edge_got.at[0], edge_send.at[1], edge_recv.at[0], ((chan + 1) % 4, slab))

    def weight_copy(i):
        return remote((w_mine, w_pair)[i], w_got.at[i], w_send.at[i], w_recv.at[i], (to_core, to_partner)[i])

    def each(first, last, body):
        def step(order, carry):
            body(tile_of(order))
            return carry

        lax.fori_loop(first, last, step, 0)

    def fetch(t):
        for slot in range(4):
            pixels(t, slot).start()

    def moments(t, first):
        pixels_wait(t, first // 2)

        def block(index, carry):
            slot = first + index // 2
            half = index % 2
            start = pl.multiple_of(half * 32, 32)
            totals = [None] * MOMENTS
            for c in range(chans):
                x = pix[t, slot, c, pl.ds(start, 32), :]
                for k in range(MOMENTS):
                    term = coef[k * chans + c] * x
                    totals[k] = term if c == 0 else totals[k] + term
            for k in range(MOMENTS):
                part[t, slot, half, k] = totals[k]
            return carry

        lax.fori_loop(0, 4, block, 0)

    def make_early(t):
        moments(t, 0)
        moments(t, 2)

    def make(t):
        moments(t, 0)
        core_copy(t).start()
        moments(t, 2)

    def join(t):
        core_copy(t).wait_recv()
        for side in range(2):
            for half in range(2):
                for k in range(MOMENTS):
                    part[t, 2 + side, half, k] = part[t, 2 + side, half, k] + got[t, side, half, k]
        far_copy(t).start()
        direct_copy(t).start()

    lane_of = lax.broadcasted_iota(jnp.int32, (16, LANES), 1)

    def pack(index, side, first):
        for k in range(MOMENTS):
            packed = jnp.zeros((16, LANES), F32)
            for group in range(4):
                piece = rows[index, k, pl.ds(16 * group, 16), :]
                shift = (32 * group - first) % LANES
                piece = piece if shift == 0 else pltpu.roll(piece, shift, 1)
                packed = jnp.where(lane_of // 32 == group, piece, packed)
            edge_mine[side, k] = packed

    def unpack(index, side, first):
        for k in range(MOMENTS):
            packed = edge_got[side, k]
            for group in range(4):
                shift = (first - 32 * group) % LANES
                piece = packed if shift == 0 else pltpu.roll(packed, shift, 1)
                rows[index, k, pl.ds(16 * group, 16), :] = jnp.where(lane_of // 32 == first // 32, piece, 0.0)

    def row_sum(k, pieces):
        high, low = halves(jnp.concatenate(pieces, axis=0))
        band = row_band[k]
        return jnp.dot(band, high, preferred_element_type=F32) + jnp.dot(band, low, preferred_element_type=F32)

    def relay(t):
        direct_copy(t).wait_recv()
        to_other[t] = part[t, 3, half_other] + from_direct[t]

        @pl.when(inside)
        def _():
            other_copy(t).start()

    def give_rows(t):
        far_copy(t).wait_recv()
        blank = jnp.zeros((32, LANES), F32)
        for k in range(MOMENTS):
            to_direct[t, k] = row_sum(k, [part[t, 3, 0, k], part[t, 3, 1, k], from_same_far[t, k], blank])
        row_copy(t).start()

    def take_rows(t):
        own_copy(t).wait_recv()

        @pl.when(inside)
        def _():
            other_copy(t).wait_recv()

        sums = [
            row_sum(k, [part[t, 2, 0, k], part[t, 2, 1, k], from_same_own[t, k], from_other[t, k]])
            for k in range(MOMENTS)
        ]
        row_copy(t).wait_recv()
        for k in range(MOMENTS):
            rows[t + 1, k] = sums[k] + from_rows[t, k]

    def finish(t, scales):
        for k in range(MOMENTS):
            wide = jnp.concatenate([rows[t, k], rows[t + 1, k], rows[t + 2, k]], axis=1)
            high, low = halves(wide)
            band = col_band[k]
            total = jnp.dot(high, band, preferred_element_type=F32) + jnp.dot(low, band, preferred_element_type=F32)
            start = pl.multiple_of(t * LANES, LANES)
            out[k, :, pl.ds(start, LANES)] = (total.reshape(8, 8, LANES) * scales[k][None]).reshape(64, LANES)

    barrier = pltpu.get_barrier_semaphore()

    def call(semaphore, where):
        pl.semaphore_signal(semaphore, inc=1, device_id=where, device_id_type=MESH)

    @pl.when(caller)
    def _():
        for friend in (to_core, to_partner, to_wrap):
            call(barrier, friend)

    @pl.when(callee)
    def _():
        call(barrier, to_far_core)

    @pl.when(jnp.logical_and(callee, inside))
    def _():
        call(barrier, to_wrap_other)

    each(0, tiles, fetch)

    weight_sum = F32(0)
    for c in range(chans):
        weight = weights[c].astype(F32)
        weight_sum = weight_sum + weight
        offset = offsets[c]
        value = weight
        for k in range(MOMENTS):
            coef[k * chans + c] = value
            value = value * offset
    w_mine[...] = jnp.full((8, LANES), weight_sum, F32)

    near = lax.broadcasted_iota(jnp.int32, (64, LANES), 0)
    lane = lax.broadcasted_iota(jnp.int32, (64, LANES), 1)
    same_shift = jnp.where(odd == 1, -96, 0)
    other_shift = jnp.where(at_edge, 1000, jnp.where(odd == 1, -32, -128))
    place = lane + jnp.where(lane < 64, 0, jnp.where(lane < 96, same_shift, other_shift))
    row_gap = jnp.abs(place - near)
    for k in range(MOMENTS):
        row_band[k] = jnp.where(row_gap <= reach[k], 1.0, 0.0).astype(BF16)

    @pl.when(callee)
    def _():
        pl.semaphore_wait(barrier, 4)
        for friend in (to_core, to_partner, to_wrap):
            call(ready, friend)

    moments(tile_of(0), 0)

    @pl.when(caller)
    def _():
        pl.semaphore_wait(ready, 3)

    weight_copy(0).start()
    core_copy(tile_of(0)).start()
    moments(tile_of(0), 2)

    def making(order, carry):
        t = tile_of(order)
        moments(t, 0)
        core_copy(t).start()
        join(tile_of(order - 1))
        moments(t, 2)
        return carry

    lax.fori_loop(1, 2, making, 0)
    weight_copy(0).wait_recv()
    w_pair[...] = w_mine[...] + w_got[0]
    lax.fori_loop(2, 3, making, 0)
    weight_copy(1).start()
    lax.fori_loop(3, tiles, making, 0)

    col_gap = jnp.abs(
        lax.broadcasted_iota(jnp.int32, (3 * LANES, LANES), 0) - LANES
        - lax.broadcasted_iota(jnp.int32, (3 * LANES, LANES), 1)
    )
    for k in range(MOMENTS):
        col_band[k] = jnp.where(col_gap <= reach[k], 1.0, 0.0).astype(BF16)

    @pl.when(at_edge)
    def _():
        from_other[...] = jnp.zeros_like(from_other)

    @pl.when(chan == 0)
    def _():
        rows[0] = jnp.zeros((MOMENTS, 64, LANES), F32)

    @pl.when(chan == 3)
    def _():
        rows[tiles + 1] = jnp.zeros((MOMENTS, 64, LANES), F32)

    join(tile_of(tiles - 1))

    @pl.when(jnp.logical_and(caller, inside))
    def _():
        pl.semaphore_wait(barrier, 1)
        call(other_ready, to_wrap_other)

    @pl.when(jnp.logical_and(callee, inside))
    def _():
        pl.semaphore_wait(other_ready, 1)

    def passing(t):
        relay(t)
        own_copy(t).start()
        give_rows(t)

    def relaying(t):
        relay(t)
        own_copy(t).start()

    early = 2
    middle = max(early, (5 * tiles) // 8)
    each(0, middle, passing)
    each(middle, tiles, relaying)
    each(0, early, take_rows)

    @pl.when(chan > 0)
    def _():
        pack(1, 0, 0)
        left_edge().start()

    @pl.when(chan < 3)
    def _():
        pack(tiles, 1, 96)
        right_edge().start()

    each(middle, tiles, give_rows)

    weight_copy(1).wait_recv()
    total = w_pair[...] + w_got[1]
    scales = [1.0 / (total * (2 * reach[k] + 1).astype(F32)) for k in range(MOMENTS)]

    @pl.when(chan < 3)
    def _():
        left_edge().wait_recv()
        unpack(tiles + 1, 1, 0)

    def finishing(order, carry):
        t = tile_of(order)
        take_rows(t)
        finish(t + 1, scales)
        return carry

    lax.fori_loop(early, tiles, finishing, 0)

    @pl.when(chan > 0)
    def _():
        right_edge().wait_recv()
        unpack(0, 0, 96)

    finish(1, scales)
    finish(0, scales)

    def sent(buffer, send):
        pltpu.make_async_copy(buffer, buffer, send).wait()

    sent(got, core_send)
    sent(from_same_far, far_send)
    sent(from_same_own, own_send)
    sent(from_direct, dir_send)
    sent(from_rows, row_send)

    @pl.when(inside)
    def _():
        sent(from_other, oth_send)

    for i in range(2):
        weight_copy(i).wait_send()

    @pl.when(chan > 0)
    def _():
        left_edge().wait_send()

    @pl.when(chan < 3)
    def _():
        right_edge().wait_send()


def solution(mesh):
    slabs = mesh.shape["slab"]

    def body(beam, weights, offsets, reach):
        chans, height, width = beam.shape
        tiles = width // (4 * LANES)
        halo = (tiles, MOMENTS, 32, LANES)
        full = (MOMENTS, 64, LANES)
        dma = pltpu.SemaphoreType.DMA
        smem = pl.BlockSpec(memory_space=pltpu.SMEM)
        return pl.pallas_call(
            functools.partial(kernel, slabs, tiles, chans),
            out_shape=pltpu.VMEM((MOMENTS, height, width // 4), F32),
            in_specs=[pl.BlockSpec(memory_space=pl.ANY), smem, smem, smem],
            out_specs=pl.BlockSpec(memory_space=pltpu.VMEM),
            scratch_shapes=[
                pltpu.VMEM((tiles, 4, chans, 64, LANES), F32),
                pltpu.VMEM((tiles, 4, 2, MOMENTS, 32, LANES), F32),
                pltpu.VMEM((tiles, 2, 2, MOMENTS, 32, LANES), F32),
                pltpu.VMEM(halo, F32),
                pltpu.VMEM(halo, F32),
                pltpu.VMEM(halo, F32),
                pltpu.VMEM(halo, F32),
                pltpu.VMEM(halo, F32),
                pltpu.VMEM((tiles, *full), F32),
                pltpu.VMEM((tiles, *full), F32),
                pltpu.VMEM((tiles + 2, *full), F32),
                pltpu.VMEM((MOMENTS, 64, LANES), BF16),
                pltpu.VMEM((MOMENTS, 3 * LANES, LANES), BF16),
                pltpu.SMEM((MOMENTS * chans,), F32),
                pltpu.VMEM((8, LANES), F32),
                pltpu.VMEM((8, LANES), F32),
                pltpu.VMEM((2, 8, LANES), F32),
                pltpu.VMEM((2, MOMENTS, 16, LANES), F32),
                pltpu.VMEM((2, MOMENTS, 16, LANES), F32),
                dma((tiles, 2)),
                dma, dma((tiles,)),
                dma, dma((tiles,)),
                dma, dma((tiles,)),
                dma, dma((tiles,)),
                dma, dma((tiles,)),
                dma, dma((tiles,)),
                dma((2,)), dma((2,)),
                dma((2,)), dma((2,)),
                pltpu.SemaphoreType.REGULAR, pltpu.SemaphoreType.REGULAR,
            ],
            compiler_params=pltpu.CompilerParams(
                collective_id=0, has_side_effects=True, vmem_limit_bytes=60 * 1024 * 1024
            ),
        )(beam, weights, offsets, reach)

    placed = (P("chan", "slab", None), P("chan"), P("chan"), P())
    return jax.shard_map(
        body, mesh=mesh, in_specs=placed, out_specs=P(None, "slab", "chan"), check_vma=False
    )
```

```python
import functools

import jax
import jax.numpy as jnp
from jax import lax
from jax.experimental import pallas as pl
from jax.experimental.pallas import tpu as pltpu
from jax.sharding import PartitionSpec as P

MESH = pl.DeviceIdType.MESH
MOMENTS = 5
HW = 32
LANES = 128
F32 = jnp.float32
BF16 = jnp.bfloat16


def halves(value):
    high = value.astype(BF16)
    low = (value - high.astype(F32)).astype(BF16)
    return high, low


def kernel(
    slabs, tiles, chans,
    beam, weights, offsets, reach, out,
    pix, part, got, raw_got, same_got, other_got, edge_same, edge_other, to_direct, from_rows,
    rows, row_band, col_band, coef, w_mine, w_pair, w_got, edge_mine, edge_got,
    pix_sem, core_send, core_recv, raw_send, raw_recv, same_send, same_recv, other_send, other_recv,
    es_send, es_recv, eo_send, eo_recv, row_send, row_recv,
    edge_send, edge_recv, w_send, w_recv, ready, other_ready,
):
    chan = lax.axis_index("chan")
    slab = lax.axis_index("slab")
    odd = slab % 2
    partner = (chan + 2) % 4
    other_core = chan + 1 - 2 * (chan % 2)
    far_core = 3 - chan
    same_slab = slab + 1 - 2 * odd
    other_slab = (slab + slabs - 1 + 2 * odd) % slabs
    half_same = 1 - odd
    half_other = odd
    to_core = (other_core, slab)
    to_partner = (partner, slab)
    to_far_core = (far_core, slab)
    to_wrap = (partner, same_slab)
    to_wrap_other = (partner, other_slab)
    caller = jnp.logical_or(chan == 0, chan == 3)
    callee = jnp.logical_not(caller)
    at_edge = jnp.logical_or(slab == 0, slab == slabs - 1)
    inside = jnp.logical_not(at_edge)

    inner = (tiles - 2) // 2
    OWN, OTH = 2, 3

    def away(i):
        return (1 + i) * (1 - odd) + (tiles - 2 - i) * odd

    def home(i):
        return (1 + i) * odd + (tiles - 2 - i) * (1 - odd)

    edge_tile = (0, tiles - 1)

    def pixels(t, slot):
        quarter = (other_core, far_core, chan, partner)[slot]
        start = pl.multiple_of((quarter * tiles + t) * LANES, LANES)
        return pltpu.make_async_copy(beam.at[:, :, pl.ds(start, LANES)], pix.at[t, slot], pix_sem.at[t, slot // 2])

    def pixels_wait(t, pair):
        two = pix.at[t, pl.ds(2 * pair, 2)]
        pltpu.make_async_copy(two, two, pix_sem.at[t, pair]).wait()

    def remote(src, dst, send, recv, where):
        return pltpu.make_async_remote_copy(
            src_ref=src, dst_ref=dst, send_sem=send, recv_sem=recv, device_id=where, device_id_type=MESH
        )

    def core_copy(t):
        return remote(part.at[t, pl.ds(0, 2)], got.at[t], core_send, core_recv.at[t], to_core)

    def raw_copy(t, slot):
        return remote(part.at[t, slot], raw_got.at[t], raw_send, raw_recv.at[t], to_partner)

    def same_copy(t, slot):
        return remote(part.at[t, slot, half_same], same_got.at[t], same_send, same_recv.at[t], to_wrap)

    def other_copy(t, slot):
        return remote(part.at[t, slot, half_other], other_got.at[t], other_send, other_recv.at[t], to_wrap_other)

    def edge_same_copy(e, slot):
        src = part.at[edge_tile[e], slot, half_same]
        return remote(src, edge_same.at[e, slot - 2], es_send, es_recv.at[e, slot - 2], to_wrap)

    def edge_other_copy(e, slot):
        src = part.at[edge_tile[e], slot, half_other]
        return remote(src, edge_other.at[e, slot - 2], eo_send, eo_recv.at[e, slot - 2], to_wrap_other)

    def edge_row_copy(e):
        t = edge_tile[e]
        return remote(to_direct.at[t], from_rows.at[e], row_send, row_recv.at[t], to_partner)

    def row_copy(t):
        return remote(to_direct.at[t], rows.at[t + 1], row_send, row_recv.at[t], to_partner)

    def left_edge():
        return remote(edge_mine.at[0], edge_got.at[1], edge_send.at[0], edge_recv.at[1], ((chan + 3) % 4, slab))

    def right_edge():
        return remote(edge_mine.at[1], edge_got.at[0], edge_send.at[1], edge_recv.at[0], ((chan + 1) % 4, slab))

    def weight_copy(i):
        return remote((w_mine, w_pair)[i], w_got.at[i], w_send.at[i], w_recv.at[i], (to_core, to_partner)[i])

    def fetch(t):
        for slot in range(4):
            pixels(t, slot).start()

    def moments(t, first):
        pixels_wait(t, first // 2)

        def block(index, carry):
            slot = first + index // 2
            half = index % 2
            start = pl.multiple_of(half * 32, 32)
            totals = [None] * MOMENTS
            for c in range(chans):
                x = pix[t, slot, c, pl.ds(start, 32), :]
                for k in range(MOMENTS):
                    term = coef[k * chans + c] * x
                    totals[k] = term if c == 0 else totals[k] + term
            for k in range(MOMENTS):
                part[t, slot, half, k] = totals[k]
            return carry

        lax.fori_loop(0, 4, block, 0)

    def join(t):
        core_copy(t).wait_recv()

        def add(index, carry):
            side = index // 2
            half = index % 2
            for k in range(MOMENTS):
                part[t, 2 + side, half, k] = part[t, 2 + side, half, k] + got[t, side, half, k]
            return carry

        lax.fori_loop(0, 4, add, 0)

    def complete(t, slot):
        raw_copy(t, slot).wait_recv()
        for half in range(2):
            for k in range(MOMENTS):
                part[t, slot, half, k] = part[t, slot, half, k] + raw_got[t, half, k]

        @pl.when(inside)
        def _():
            other_copy(t, slot).start()

        same_copy(t, slot).start()

    lane_of = lax.broadcasted_iota(jnp.int32, (16, LANES), 1)

    def pack(index, side, first):
        for k in range(MOMENTS):
            packed = jnp.zeros((16, LANES), F32)
            for group in range(4):
                piece = rows[index, k, pl.ds(16 * group, 16), :]
                shift = (32 * group - first) % LANES
                piece = piece if shift == 0 else pltpu.roll(piece, shift, 1)
                packed = jnp.where(lane_of // 32 == group, piece, packed)
            edge_mine[side, k] = packed

    def unpack(index, side, first):
        for k in range(MOMENTS):
            packed = edge_got[side, k]
            for group in range(4):
                shift = (first - 32 * group) % LANES
                piece = packed if shift == 0 else pltpu.roll(packed, shift, 1)
                rows[index, k, pl.ds(16 * group, 16), :] = jnp.where(lane_of // 32 == first // 32, piece, 0.0)

    def row_sum(k, pieces):
        high, low = halves(jnp.concatenate(pieces, axis=0))
        band = row_band[k]
        return jnp.dot(band, high, preferred_element_type=F32) + jnp.dot(band, low, preferred_element_type=F32)

    def tile_rows(t, slot, dst, at):
        same_copy(t, slot).wait_recv()

        @pl.when(inside)
        def _():
            other_copy(t, slot).wait_recv()

        for k in range(MOMENTS):
            dst[at, k] = row_sum(k, [part[t, slot, 0, k], part[t, slot, 1, k], same_got[t, k], other_got[t, k]])

    def give_back(t):
        tile_rows(t, OTH, to_direct, t)
        row_copy(t).start()

    def edge_sums(e, slot):
        t = edge_tile[e]
        theirs = OWN + OTH - slot
        edge_same_copy(e, theirs).wait_recv()

        @pl.when(inside)
        def _():
            edge_other_copy(e, theirs).wait_recv()

        i = theirs - 2
        return [
            row_sum(k, [part[t, slot, 0, k], part[t, slot, 1, k], edge_same[e, i, k], edge_other[e, i, k]])
            for k in range(MOMENTS)
        ]

    def edge_give(e):
        sums = edge_sums(e, OTH)
        for k in range(MOMENTS):
            to_direct[edge_tile[e], k] = sums[k]
        edge_row_copy(e).start()

    def edge_take(e):
        sums = edge_sums(e, OWN)
        edge_row_copy(e).wait_recv()
        for k in range(MOMENTS):
            rows[edge_tile[e] + 1, k] = sums[k] + from_rows[e, k]

    def finish(t, scales):
        start = pl.multiple_of(t * LANES, LANES)
        for k in range(MOMENTS):
            wide = jnp.concatenate([rows[t, k], rows[t + 1, k], rows[t + 2, k]], axis=1)
            high, low = halves(wide)
            band = col_band[k]
            total = jnp.dot(high, band, preferred_element_type=F32) + jnp.dot(low, band, preferred_element_type=F32)
            out[k, :, pl.ds(start, LANES)] = (total.reshape(8, 8, LANES) * scales[k][None]).reshape(64, LANES)

    barrier = pltpu.get_barrier_semaphore()

    def call(semaphore, where):
        pl.semaphore_signal(semaphore, inc=1, device_id=where, device_id_type=MESH)

    @pl.when(caller)
    def _():
        for friend in (to_core, to_partner, to_wrap):
            call(barrier, friend)

    @pl.when(callee)
    def _():
        call(barrier, to_far_core)

    @pl.when(jnp.logical_and(callee, inside))
    def _():
        call(barrier, to_wrap_other)

    order = []
    for i in range(max(inner, 2)):
        if i < inner:
            order.append(("away", away(i)))
        if i < 2:
            order.append(("edge", edge_tile[i]))
        if i < inner:
            order.append(("home", home(i)))
    ahead = 3
    for _, t in order[:ahead]:
        fetch(t)

    weight_sum = F32(0)
    for c in range(chans):
        weight = weights[c].astype(F32)
        weight_sum = weight_sum + weight
        offset = offsets[c]
        value = weight
        for k in range(MOMENTS):
            coef[k * chans + c] = value
            value = value * offset
    w_mine[...] = jnp.full((8, LANES), weight_sum, F32)

    near = lax.broadcasted_iota(jnp.int32, (64, LANES), 0)
    lane = lax.broadcasted_iota(jnp.int32, (64, LANES), 1)
    same_shift = jnp.where(odd == 1, -96, 0)
    other_shift = jnp.where(at_edge, 1000, jnp.where(odd == 1, -32, -128))
    place = lane + jnp.where(lane < 64, 0, jnp.where(lane < 96, same_shift, other_shift))
    row_gap = jnp.abs(place - near)
    for k in range(MOMENTS):
        row_band[k] = jnp.where(row_gap <= reach[k], 1.0, 0.0).astype(BF16)

    @pl.when(callee)
    def _():
        pl.semaphore_wait(barrier, 4)
        for friend in (to_core, to_partner, to_wrap):
            call(ready, friend)

    def joined(kind, t):
        join(t)
        if kind == "away":
            raw_copy(t, OWN).start()
        elif kind == "home":
            raw_copy(t, OTH).start()
        elif kind == "edge":
            edge_same_copy(edge_tile.index(t), OWN).start()
            edge_same_copy(edge_tile.index(t), OTH).start()

    for i, (kind, t) in enumerate(order):
        moments(t, 0)
        if i == 0:

            @pl.when(caller)
            def _():
                pl.semaphore_wait(ready, 3)

            weight_copy(0).start()
        core_copy(t).start()
        if i + ahead < len(order):
            fetch(order[i + ahead][1])
        if i > 0:
            joined(*order[i - 1])
        moments(t, 2)
        if i == 1:
            weight_copy(0).wait_recv()
            w_pair[...] = w_mine[...] + w_got[0]
        if i == 2:
            weight_copy(1).start()
        if i == 2 + inner:
            col_gap = jnp.abs(
                lax.broadcasted_iota(jnp.int32, (3 * LANES, LANES), 0) - LANES
                - lax.broadcasted_iota(jnp.int32, (3 * LANES, LANES), 1)
            )
            for k in range(MOMENTS):
                col_band[k] = jnp.where(col_gap <= reach[k], 1.0, 0.0).astype(BF16)
    joined(*order[-1])

    @pl.when(at_edge)
    def _():
        other_got[...] = jnp.zeros_like(other_got)
        edge_other[...] = jnp.zeros_like(edge_other)

    @pl.when(chan == 0)
    def _():
        rows[0] = jnp.zeros((MOMENTS, 64, LANES), F32)

    @pl.when(chan == 3)
    def _():
        rows[tiles + 1] = jnp.zeros((MOMENTS, 64, LANES), F32)

    @pl.when(jnp.logical_and(caller, inside))
    def _():
        pl.semaphore_wait(barrier, 1)
        call(other_ready, to_wrap_other)

    @pl.when(jnp.logical_and(callee, inside))
    def _():
        pl.semaphore_wait(other_ready, 1)

    def edge_others(slot):
        @pl.when(inside)
        def _():
            for e in range(2):
                edge_other_copy(e, slot).start()

    def complete_pair(i):
        complete(away(i), OTH)
        complete(home(i), OWN)

    def rows_pair(i):
        give_back(away(i))
        tile_rows(home(i), OWN, rows, home(i) + 1)

    edge_others(OWN)
    complete_pair(0)
    edge_others(OTH)
    for i in range(1, inner - 1):
        complete_pair(i)
    for e in range(2):
        edge_give(e)
    rows_pair(0)
    if inner > 1:
        complete_pair(inner - 1)
    for i in range(1, inner - 1):
        rows_pair(i)
    for e in range(2):
        edge_take(e)

    @pl.when(chan > 0)
    def _():
        pack(1, 0, 0)
        left_edge().start()

    @pl.when(chan < 3)
    def _():
        pack(tiles, 1, 96)
        right_edge().start()

    if inner > 1:
        rows_pair(inner - 1)

    weight_copy(1).wait_recv()
    total = w_pair[...] + w_got[1]
    scales = [1.0 / (total * (2 * reach[k] + 1).astype(F32)) for k in range(MOMENTS)]

    @pl.when(chan < 3)
    def _():
        left_edge().wait_recv()
        unpack(tiles + 1, 1, 0)

    @pl.when(chan > 0)
    def _():
        right_edge().wait_recv()
        unpack(0, 0, 96)

    out_step = 1 - 2 * odd

    def last_steps(i, carry):
        finish(home(i) + out_step, scales)
        row_copy(away(i)).wait_recv()
        finish(away(i) - out_step, scales)
        return carry

    lax.fori_loop(0, inner, last_steps, 0)
    finish(home(inner - 1), scales)
    finish(away(inner - 1), scales)

    def sent(buffer, send):
        pltpu.make_async_copy(buffer, buffer, send).wait()

    middle = pl.ds(1, tiles - 2)
    sent(got, core_send)
    sent(raw_got.at[middle], raw_send)
    sent(same_got.at[middle], same_send)
    sent(edge_same, es_send)
    sent(rows.at[pl.ds(0, inner + 2)], row_send)

    @pl.when(inside)
    def _():
        sent(other_got.at[middle], other_send)
        sent(edge_other, eo_send)

    for i in range(2):
        weight_copy(i).wait_send()

    @pl.when(chan > 0)
    def _():
        left_edge().wait_send()

    @pl.when(chan < 3)
    def _():
        right_edge().wait_send()


def solution(mesh):
    slabs = mesh.shape["slab"]

    def body(beam, weights, offsets, reach):
        chans, height, width = beam.shape
        tiles = width // (4 * LANES)
        halo = (MOMENTS, 32, LANES)
        full = (MOMENTS, 64, LANES)
        dma = pltpu.SemaphoreType.DMA
        smem = pl.BlockSpec(memory_space=pltpu.SMEM)
        return pl.pallas_call(
            functools.partial(kernel, slabs, tiles, chans),
            out_shape=pltpu.VMEM((MOMENTS, height, width // 4), F32),
            in_specs=[pl.BlockSpec(memory_space=pl.ANY), smem, smem, smem],
            out_specs=pl.BlockSpec(memory_space=pltpu.VMEM),
            scratch_shapes=[
                pltpu.VMEM((tiles, 4, chans, 64, LANES), F32),
                pltpu.VMEM((tiles, 4, 2, *halo), F32),
                pltpu.VMEM((tiles, 2, 2, *halo), F32),
                pltpu.VMEM((tiles, 2, *halo), F32),
                pltpu.VMEM((tiles, *halo), F32),
                pltpu.VMEM((tiles, *halo), F32),
                pltpu.VMEM((2, 2, *halo), F32),
                pltpu.VMEM((2, 2, *halo), F32),
                pltpu.VMEM((tiles, *full), F32),
                pltpu.VMEM((2, *full), F32),
                pltpu.VMEM((tiles + 2, *full), F32),
                pltpu.VMEM((MOMENTS, 64, LANES), BF16),
                pltpu.VMEM((MOMENTS, 3 * LANES, LANES), BF16),
                pltpu.SMEM((MOMENTS * chans,), F32),
                pltpu.VMEM((8, LANES), F32),
                pltpu.VMEM((8, LANES), F32),
                pltpu.VMEM((2, 8, LANES), F32),
                pltpu.VMEM((2, MOMENTS, 16, LANES), F32),
                pltpu.VMEM((2, MOMENTS, 16, LANES), F32),
                dma((tiles, 2)),
                dma, dma((tiles,)),
                dma, dma((tiles,)),
                dma, dma((tiles,)),
                dma, dma((tiles,)),
                dma, dma((2, 2)),
                dma, dma((2, 2)),
                dma, dma((tiles,)),
                dma((2,)), dma((2,)),
                dma((2,)), dma((2,)),
                pltpu.SemaphoreType.REGULAR, pltpu.SemaphoreType.REGULAR,
            ],
            compiler_params=pltpu.CompilerParams(
                collective_id=0, has_side_effects=True, vmem_limit_bytes=60 * 1024 * 1024
            ),
        )(beam, weights, offsets, reach)

    placed = (P("chan", "slab", None), P("chan"), P("chan"), P())
    return jax.shard_map(
        body, mesh=mesh, in_specs=placed, out_specs=P(None, "slab", "chan"), check_vma=False
    )
```

```python
import functools

import jax
import jax.numpy as jnp
from jax import lax
from jax.experimental import pallas as pl
from jax.experimental.pallas import tpu as pltpu
from jax.sharding import PartitionSpec as P

MESH = pl.DeviceIdType.MESH
MOMENTS = 5
HW = 32
LANES = 128
F32 = jnp.float32
BF16 = jnp.bfloat16


def halves(value):
    high = value.astype(BF16)
    low = (value - high.astype(F32)).astype(BF16)
    return high, low


def kernel(
    slabs, tiles, chans,
    beam, weights, offsets, reach, out,
    pix, part, got, raw_got, same_got, other_got, edge_same, edge_other, to_direct, from_rows,
    rows, row_band, col_band, coef, w_mine, w_pair, w_got, edge_mine, edge_got,
    pix_sem, core_send, core_recv, raw_send, raw_recv, same_send, same_recv, other_send, other_recv,
    es_send, es_recv, eo_send, eo_recv, row_send, row_recv,
    edge_send, edge_recv, w_send, w_recv, ready, other_ready,
):
    chan = lax.axis_index("chan")
    slab = lax.axis_index("slab")
    odd = slab % 2
    partner = (chan + 2) % 4
    other_core = chan + 1 - 2 * (chan % 2)
    far_core = 3 - chan
    same_slab = slab + 1 - 2 * odd
    other_slab = (slab + slabs - 1 + 2 * odd) % slabs
    half_same = 1 - odd
    half_other = odd
    to_core = (other_core, slab)
    to_partner = (partner, slab)
    to_far_core = (far_core, slab)
    to_wrap = (partner, same_slab)
    to_wrap_other = (partner, other_slab)
    caller = jnp.logical_or(chan == 0, chan == 3)
    callee = jnp.logical_not(caller)
    at_edge = jnp.logical_or(slab == 0, slab == slabs - 1)
    inside = jnp.logical_not(at_edge)

    inner = (tiles - 2) // 2
    OWN, OTH = 2, 3

    def away(i):
        return (1 + i) * (1 - odd) + (tiles - 2 - i) * odd

    def home(i):
        return (1 + i) * odd + (tiles - 2 - i) * (1 - odd)

    edge_tile = (0, tiles - 1)

    def pixels(t, slot):
        quarter = (other_core, far_core, chan, partner)[slot]
        start = pl.multiple_of((quarter * tiles + t) * LANES, LANES)
        return pltpu.make_async_copy(beam.at[:, :, pl.ds(start, LANES)], pix.at[t, slot], pix_sem.at[t, slot // 2])

    def pixels_wait(t, pair):
        two = pix.at[t, pl.ds(2 * pair, 2)]
        pltpu.make_async_copy(two, two, pix_sem.at[t, pair]).wait()

    def remote(src, dst, send, recv, where):
        return pltpu.make_async_remote_copy(
            src_ref=src, dst_ref=dst, send_sem=send, recv_sem=recv, device_id=where, device_id_type=MESH
        )

    def core_copy(t):
        return remote(part.at[t, pl.ds(0, 2)], got.at[t], core_send, core_recv.at[t], to_core)

    def raw_copy(t, slot):
        return remote(part.at[t, slot], raw_got.at[t], raw_send, raw_recv.at[t], to_partner)

    def same_copy(t, slot):
        return remote(part.at[t, slot, half_same], same_got.at[t], same_send, same_recv.at[t], to_wrap)

    def other_copy(t, slot):
        return remote(part.at[t, slot, half_other], other_got.at[t], other_send, other_recv.at[t], to_wrap_other)

    def edge_same_copy(e, slot):
        src = part.at[edge_tile[e], slot, half_same]
        return remote(src, edge_same.at[e, slot - 2], es_send, es_recv.at[e, slot - 2], to_wrap)

    def edge_other_copy(e, slot):
        src = part.at[edge_tile[e], slot, half_other]
        return remote(src, edge_other.at[e, slot - 2], eo_send, eo_recv.at[e, slot - 2], to_wrap_other)

    def edge_row_copy(e):
        t = edge_tile[e]
        return remote(to_direct.at[t], from_rows.at[e], row_send, row_recv.at[t], to_partner)

    def row_copy(t):
        return remote(to_direct.at[t], rows.at[t + 1], row_send, row_recv.at[t], to_partner)

    def left_edge():
        return remote(edge_mine.at[0], edge_got.at[1], edge_send.at[0], edge_recv.at[1], ((chan + 3) % 4, slab))

    def right_edge():
        return remote(edge_mine.at[1], edge_got.at[0], edge_send.at[1], edge_recv.at[0], ((chan + 1) % 4, slab))

    def weight_copy(i):
        return remote((w_mine, w_pair)[i], w_got.at[i], w_send.at[i], w_recv.at[i], (to_core, to_partner)[i])

    def fetch(t):
        for slot in range(4):
            pixels(t, slot).start()

    def moments(t, first):
        pixels_wait(t, first // 2)

        def block(index, carry):
            slot = first + index // 2
            half = index % 2
            start = pl.multiple_of(half * 32, 32)
            totals = [None] * MOMENTS
            for c in range(chans):
                x = pix[t, slot, c, pl.ds(start, 32), :]
                for k in range(MOMENTS):
                    term = coef[k * chans + c] * x
                    totals[k] = term if c == 0 else totals[k] + term
            for k in range(MOMENTS):
                part[t, slot, half, k] = totals[k]
            return carry

        lax.fori_loop(0, 4, block, 0)

    def join(t):
        core_copy(t).wait_recv()

        def add(index, carry):
            side = index // 2
            half = index % 2
            for k in range(MOMENTS):
                part[t, 2 + side, half, k] = part[t, 2 + side, half, k] + got[t, side, half, k]
            return carry

        lax.fori_loop(0, 4, add, 0)

    def complete(t, slot):
        raw_copy(t, slot).wait_recv()
        for half in range(2):
            for k in range(MOMENTS):
                part[t, slot, half, k] = part[t, slot, half, k] + raw_got[t, half, k]

        @pl.when(inside)
        def _():
            other_copy(t, slot).start()

        same_copy(t, slot).start()

    lane_of = lax.broadcasted_iota(jnp.int32, (16, LANES), 1)

    def pack(index, side, first):
        for k in range(MOMENTS):
            packed = jnp.zeros((16, LANES), F32)
            for group in range(4):
                piece = rows[index, k, pl.ds(16 * group, 16), :]
                shift = (32 * group - first) % LANES
                piece = piece if shift == 0 else pltpu.roll(piece, shift, 1)
                packed = jnp.where(lane_of // 32 == group, piece, packed)
            edge_mine[side, k] = packed

    def unpack(index, side, first):
        for k in range(MOMENTS):
            packed = edge_got[side, k]
            for group in range(4):
                shift = (first - 32 * group) % LANES
                piece = packed if shift == 0 else pltpu.roll(packed, shift, 1)
                rows[index, k, pl.ds(16 * group, 16), :] = jnp.where(lane_of // 32 == first // 32, piece, 0.0)

    def row_sum(k, pieces):
        high, low = halves(jnp.concatenate(pieces, axis=0))
        band = row_band[k]
        return jnp.dot(band, high, preferred_element_type=F32) + jnp.dot(band, low, preferred_element_type=F32)

    def tile_rows(t, slot, dst, at):
        same_copy(t, slot).wait_recv()

        @pl.when(inside)
        def _():
            other_copy(t, slot).wait_recv()

        for k in range(MOMENTS):
            dst[at, k] = row_sum(k, [part[t, slot, 0, k], part[t, slot, 1, k], same_got[t, k], other_got[t, k]])

    def give_back(t):
        tile_rows(t, OTH, to_direct, t)
        row_copy(t).start()

    def edge_sums(e, slot):
        t = edge_tile[e]
        theirs = OWN + OTH - slot
        edge_same_copy(e, theirs).wait_recv()

        @pl.when(inside)
        def _():
            edge_other_copy(e, theirs).wait_recv()

        i = theirs - 2
        return [
            row_sum(k, [part[t, slot, 0, k], part[t, slot, 1, k], edge_same[e, i, k], edge_other[e, i, k]])
            for k in range(MOMENTS)
        ]

    def edge_give(e):
        sums = edge_sums(e, OTH)
        for k in range(MOMENTS):
            to_direct[edge_tile[e], k] = sums[k]
        edge_row_copy(e).start()

    def edge_take(e):
        sums = edge_sums(e, OWN)
        edge_row_copy(e).wait_recv()
        for k in range(MOMENTS):
            rows[edge_tile[e] + 1, k] = sums[k] + from_rows[e, k]

    def finish(t, scales):
        start = pl.multiple_of(t * LANES, LANES)
        for k in range(MOMENTS):
            wide = jnp.concatenate([rows[t, k], rows[t + 1, k], rows[t + 2, k]], axis=1)
            high, low = halves(wide)
            band = col_band[k]
            total = jnp.dot(high, band, preferred_element_type=F32) + jnp.dot(low, band, preferred_element_type=F32)
            out[k, :, pl.ds(start, LANES)] = (total.reshape(8, 8, LANES) * scales[k][None]).reshape(64, LANES)

    barrier = pltpu.get_barrier_semaphore()

    def call(semaphore, where):
        pl.semaphore_signal(semaphore, inc=1, device_id=where, device_id_type=MESH)

    @pl.when(caller)
    def _():
        for friend in (to_core, to_partner, to_wrap):
            call(barrier, friend)

    @pl.when(callee)
    def _():
        call(barrier, to_far_core)

    @pl.when(jnp.logical_and(callee, inside))
    def _():
        call(barrier, to_wrap_other)

    order = []
    for i in range(max(inner, 2)):
        if i < inner:
            order.append(("away", i, away(i)))
        if i < 2:
            order.append(("edge", i, edge_tile[i]))
        if i < inner:
            order.append(("home", i, home(i)))
    ahead = 3
    for _, _, t in order[:ahead]:
        fetch(t)

    weight_sum = F32(0)
    for c in range(chans):
        weight = weights[c].astype(F32)
        weight_sum = weight_sum + weight
        offset = offsets[c]
        value = weight
        for k in range(MOMENTS):
            coef[k * chans + c] = value
            value = value * offset
    w_mine[...] = jnp.full((8, LANES), weight_sum, F32)

    near = lax.broadcasted_iota(jnp.int32, (64, LANES), 0)
    lane = lax.broadcasted_iota(jnp.int32, (64, LANES), 1)
    same_shift = jnp.where(odd == 1, -96, 0)
    other_shift = jnp.where(at_edge, 1000, jnp.where(odd == 1, -32, -128))
    place = lane + jnp.where(lane < 64, 0, jnp.where(lane < 96, same_shift, other_shift))
    row_gap = jnp.abs(place - near)
    for k in range(MOMENTS):
        row_band[k] = jnp.where(row_gap <= reach[k], 1.0, 0.0).astype(BF16)

    @pl.when(callee)
    def _():
        pl.semaphore_wait(barrier, 4)
        for friend in (to_core, to_partner, to_wrap):
            call(ready, friend)

    last = inner - 1

    def joined(kind, i, t):
        join(t)
        if kind == "edge":
            edge_same_copy(i, OWN).start()
            if i == 0:
                edge_same_copy(i, OTH).start()
        elif i < last or last == 0:
            raw_copy(t, OWN if kind == "away" else OTH).start()

    for i, (kind, at, t) in enumerate(order):
        moments(t, 0)
        if i == 0:

            @pl.when(caller)
            def _():
                pl.semaphore_wait(ready, 3)

            weight_copy(0).start()
        core_copy(t).start()
        if i + ahead < len(order):
            fetch(order[i + ahead][2])
        if i > 0:
            joined(*order[i - 1])
        moments(t, 2)
        if i == 1:
            weight_copy(0).wait_recv()
            w_pair[...] = w_mine[...] + w_got[0]
        if i == 2:
            weight_copy(1).start()
        if i == 2 + inner:
            col_gap = jnp.abs(
                lax.broadcasted_iota(jnp.int32, (3 * LANES, LANES), 0) - LANES
                - lax.broadcasted_iota(jnp.int32, (3 * LANES, LANES), 1)
            )
            for k in range(MOMENTS):
                col_band[k] = jnp.where(col_gap <= reach[k], 1.0, 0.0).astype(BF16)
    joined(*order[-1])

    @pl.when(at_edge)
    def _():
        other_got[...] = jnp.zeros_like(other_got)
        edge_other[...] = jnp.zeros_like(edge_other)

    @pl.when(chan == 0)
    def _():
        rows[0] = jnp.zeros((MOMENTS, 64, LANES), F32)

    @pl.when(chan == 3)
    def _():
        rows[tiles + 1] = jnp.zeros((MOMENTS, 64, LANES), F32)

    @pl.when(jnp.logical_and(caller, inside))
    def _():
        pl.semaphore_wait(barrier, 1)
        call(other_ready, to_wrap_other)

    @pl.when(jnp.logical_and(callee, inside))
    def _():
        pl.semaphore_wait(other_ready, 1)

    def edge_others(slot):
        @pl.when(inside)
        def _():
            for e in range(2):
                edge_other_copy(e, slot).start()

    def complete_pair(i):
        complete(away(i), OTH)
        complete(home(i), OWN)

    def rows_pair(i):
        give_back(away(i))
        tile_rows(home(i), OWN, rows, home(i) + 1)

    edge_others(OWN)
    for i in range(last):
        complete(away(i), OTH)
        complete(home(i), OWN)
        if i == 0:
            raw_copy(home(last), OTH).start()
            raw_copy(away(last), OWN).start()
    for e in range(2):
        edge_give(e)

    def rows_pair(i):
        give_back(away(i))
        tile_rows(home(i), OWN, rows, home(i) + 1)

    if last > 0:
        rows_pair(0)
    complete(home(last), OWN)
    edge_same_copy(1, OTH).start()
    edge_others(OTH)
    complete(away(last), OTH)
    for i in range(1, last):
        rows_pair(i)
    give_back(away(last))
    for e in range(2):
        edge_take(e)

    @pl.when(chan > 0)
    def _():
        pack(1, 0, 0)
        left_edge().start()

    @pl.when(chan < 3)
    def _():
        pack(tiles, 1, 96)
        right_edge().start()

    tile_rows(home(last), OWN, rows, home(last) + 1)
    weight_copy(1).wait_recv()
    total = w_pair[...] + w_got[1]
    scales = [1.0 / (total * (2 * reach[k] + 1).astype(F32)) for k in range(MOMENTS)]

    @pl.when(chan < 3)
    def _():
        left_edge().wait_recv()
        unpack(tiles + 1, 1, 0)

    @pl.when(chan > 0)
    def _():
        right_edge().wait_recv()
        unpack(0, 0, 96)

    out_step = 1 - 2 * odd

    def last_steps(i, carry):
        finish(home(i) + out_step, scales)
        row_copy(away(i)).wait_recv()
        finish(away(i) - out_step, scales)
        return carry

    lax.fori_loop(0, inner, last_steps, 0)
    finish(home(inner - 1), scales)
    finish(away(inner - 1), scales)

    def sent(buffer, send):
        pltpu.make_async_copy(buffer, buffer, send).wait()

    middle = pl.ds(1, tiles - 2)
    sent(got, core_send)
    sent(raw_got.at[middle], raw_send)
    sent(same_got.at[middle], same_send)
    sent(edge_same, es_send)
    sent(rows.at[pl.ds(0, inner + 2)], row_send)

    @pl.when(inside)
    def _():
        sent(other_got.at[middle], other_send)
        sent(edge_other, eo_send)

    for i in range(2):
        weight_copy(i).wait_send()

    @pl.when(chan > 0)
    def _():
        left_edge().wait_send()

    @pl.when(chan < 3)
    def _():
        right_edge().wait_send()


def solution(mesh):
    slabs = mesh.shape["slab"]

    def body(beam, weights, offsets, reach):
        chans, height, width = beam.shape
        tiles = width // (4 * LANES)
        halo = (MOMENTS, 32, LANES)
        full = (MOMENTS, 64, LANES)
        dma = pltpu.SemaphoreType.DMA
        smem = pl.BlockSpec(memory_space=pltpu.SMEM)
        return pl.pallas_call(
            functools.partial(kernel, slabs, tiles, chans),
            out_shape=pltpu.VMEM((MOMENTS, height, width // 4), F32),
            in_specs=[pl.BlockSpec(memory_space=pl.ANY), smem, smem, smem],
            out_specs=pl.BlockSpec(memory_space=pltpu.VMEM),
            scratch_shapes=[
                pltpu.VMEM((tiles, 4, chans, 64, LANES), F32),
                pltpu.VMEM((tiles, 4, 2, *halo), F32),
                pltpu.VMEM((tiles, 2, 2, *halo), F32),
                pltpu.VMEM((tiles, 2, *halo), F32),
                pltpu.VMEM((tiles, *halo), F32),
                pltpu.VMEM((tiles, *halo), F32),
                pltpu.VMEM((2, 2, *halo), F32),
                pltpu.VMEM((2, 2, *halo), F32),
                pltpu.VMEM((tiles, *full), F32),
                pltpu.VMEM((2, *full), F32),
                pltpu.VMEM((tiles + 2, *full), F32),
                pltpu.VMEM((MOMENTS, 64, LANES), BF16),
                pltpu.VMEM((MOMENTS, 3 * LANES, LANES), BF16),
                pltpu.SMEM((MOMENTS * chans,), F32),
                pltpu.VMEM((8, LANES), F32),
                pltpu.VMEM((8, LANES), F32),
                pltpu.VMEM((2, 8, LANES), F32),
                pltpu.VMEM((2, MOMENTS, 16, LANES), F32),
                pltpu.VMEM((2, MOMENTS, 16, LANES), F32),
                dma((tiles, 2)),
                dma, dma((tiles,)),
                dma, dma((tiles,)),
                dma, dma((tiles,)),
                dma, dma((tiles,)),
                dma, dma((2, 2)),
                dma, dma((2, 2)),
                dma, dma((tiles,)),
                dma((2,)), dma((2,)),
                dma((2,)), dma((2,)),
                pltpu.SemaphoreType.REGULAR, pltpu.SemaphoreType.REGULAR,
            ],
            compiler_params=pltpu.CompilerParams(
                collective_id=0, has_side_effects=True, vmem_limit_bytes=60 * 1024 * 1024
            ),
        )(beam, weights, offsets, reach)

    placed = (P("chan", "slab", None), P("chan"), P("chan"), P())
    return jax.shard_map(
        body, mesh=mesh, in_specs=placed, out_specs=P(None, "slab", "chan"), check_vma=False
    )
```

```python
import functools

import jax
import jax.numpy as jnp
from jax import lax
from jax.experimental import pallas as pl
from jax.experimental.pallas import tpu as pltpu
from jax.sharding import PartitionSpec as P

MESH = pl.DeviceIdType.MESH
MOMENTS = 5
HW = 32
LANES = 128
F32 = jnp.float32
BF16 = jnp.bfloat16


def halves(value):
    high = value.astype(BF16)
    low = (value - high.astype(F32)).astype(BF16)
    return high, low


def kernel(
    slabs, tiles, chans,
    beam, weights, offsets, reach, out,
    pix, part, got, raw_got, same_got, other_got, edge_same, edge_other, to_direct, from_rows,
    rows, row_band, col_band, coef, w_mine, w_pair, w_got, edge_mine, edge_got,
    pix_sem, core_send, core_recv, raw_send, raw_recv, same_send, same_recv, other_send, other_recv,
    es_send, es_recv, eo_send, eo_recv, row_send, row_recv,
    edge_send, edge_recv, w_send, w_recv, ready, other_ready,
):
    chan = lax.axis_index("chan")
    slab = lax.axis_index("slab")
    odd = slab % 2
    partner = (chan + 2) % 4
    other_core = chan + 1 - 2 * (chan % 2)
    far_core = 3 - chan
    same_slab = slab + 1 - 2 * odd
    other_slab = (slab + slabs - 1 + 2 * odd) % slabs
    half_same = 1 - odd
    half_other = odd
    to_core = (other_core, slab)
    to_partner = (partner, slab)
    to_far_core = (far_core, slab)
    to_wrap = (partner, same_slab)
    to_wrap_other = (partner, other_slab)
    caller = jnp.logical_or(chan == 0, chan == 3)
    callee = jnp.logical_not(caller)
    at_edge = jnp.logical_or(slab == 0, slab == slabs - 1)
    inside = jnp.logical_not(at_edge)

    inner = (tiles - 2) // 2
    OWN, OTH = 2, 3

    def away(i):
        return (1 + i) * (1 - odd) + (tiles - 2 - i) * odd

    def home(i):
        return (1 + i) * odd + (tiles - 2 - i) * (1 - odd)

    edge_tile = (0, tiles - 1)

    def pixels(t, slot):
        quarter = (other_core, far_core, chan, partner)[slot]
        start = pl.multiple_of((quarter * tiles + t) * LANES, LANES)
        return pltpu.make_async_copy(beam.at[:, :, pl.ds(start, LANES)], pix.at[t, slot], pix_sem.at[t, slot // 2])

    def pixels_wait(t, pair):
        two = pix.at[t, pl.ds(2 * pair, 2)]
        pltpu.make_async_copy(two, two, pix_sem.at[t, pair]).wait()

    def remote(src, dst, send, recv, where):
        return pltpu.make_async_remote_copy(
            src_ref=src, dst_ref=dst, send_sem=send, recv_sem=recv, device_id=where, device_id_type=MESH
        )

    def core_copy(t):
        return remote(part.at[t, pl.ds(0, 2)], got.at[t], core_send, core_recv.at[t], to_core)

    def raw_copy(t, slot):
        return remote(part.at[t, slot], raw_got.at[t], raw_send, raw_recv.at[t], to_partner)

    def same_copy(t, slot):
        return remote(part.at[t, slot, half_same], same_got.at[t], same_send, same_recv.at[t], to_wrap)

    def other_copy(t, slot):
        return remote(part.at[t, slot, half_other], other_got.at[t], other_send, other_recv.at[t], to_wrap_other)

    def edge_same_copy(e, slot):
        src = part.at[edge_tile[e], slot, half_same]
        return remote(src, edge_same.at[e, slot - 2], es_send, es_recv.at[e, slot - 2], to_wrap)

    def edge_other_copy(e, slot):
        src = part.at[edge_tile[e], slot, half_other]
        return remote(src, edge_other.at[e, slot - 2], eo_send, eo_recv.at[e, slot - 2], to_wrap_other)

    def edge_row_copy(e):
        t = edge_tile[e]
        return remote(to_direct.at[t], from_rows.at[e], row_send, row_recv.at[t], to_partner)

    def row_copy(t):
        return remote(to_direct.at[t], rows.at[t + 1], row_send, row_recv.at[t], to_partner)

    def left_edge():
        return remote(edge_mine.at[0], edge_got.at[1], edge_send.at[0], edge_recv.at[1], ((chan + 3) % 4, slab))

    def right_edge():
        return remote(edge_mine.at[1], edge_got.at[0], edge_send.at[1], edge_recv.at[0], ((chan + 1) % 4, slab))

    def weight_copy(i):
        return remote((w_mine, w_pair)[i], w_got.at[i], w_send.at[i], w_recv.at[i], (to_core, to_partner)[i])

    def fetch(t):
        for slot in range(4):
            pixels(t, slot).start()

    def moments(t, first):
        pixels_wait(t, first // 2)

        def block(index, carry):
            slot = first + index // 2
            half = index % 2
            start = pl.multiple_of(half * 32, 32)
            totals = [None] * MOMENTS
            for c in range(chans):
                x = pix[t, slot, c, pl.ds(start, 32), :]
                for k in range(MOMENTS):
                    term = coef[k * chans + c] * x
                    totals[k] = term if c == 0 else totals[k] + term
            for k in range(MOMENTS):
                part[t, slot, half, k] = totals[k]
            return carry

        lax.fori_loop(0, 4, block, 0)

    def join(t):
        core_copy(t).wait_recv()

        def add(index, carry):
            side = index // 2
            half = index % 2
            for k in range(MOMENTS):
                part[t, 2 + side, half, k] = part[t, 2 + side, half, k] + got[t, side, half, k]
            return carry

        lax.fori_loop(0, 4, add, 0)

    def complete(t, slot):
        raw_copy(t, slot).wait_recv()
        for half in range(2):
            for k in range(MOMENTS):
                part[t, slot, half, k] = part[t, slot, half, k] + raw_got[t, half, k]

        @pl.when(inside)
        def _():
            other_copy(t, slot).start()

        same_copy(t, slot).start()

    lane_of = lax.broadcasted_iota(jnp.int32, (16, LANES), 1)

    def pack(index, side, first):
        for k in range(MOMENTS):
            packed = jnp.zeros((16, LANES), F32)
            for group in range(4):
                piece = rows[index, k, pl.ds(16 * group, 16), :]
                shift = (32 * group - first) % LANES
                piece = piece if shift == 0 else pltpu.roll(piece, shift, 1)
                packed = jnp.where(lane_of // 32 == group, piece, packed)
            edge_mine[side, k] = packed

    def unpack(index, side, first):
        for k in range(MOMENTS):
            packed = edge_got[side, k]
            for group in range(4):
                shift = (first - 32 * group) % LANES
                piece = packed if shift == 0 else pltpu.roll(packed, shift, 1)
                rows[index, k, pl.ds(16 * group, 16), :] = jnp.where(lane_of // 32 == first // 32, piece, 0.0)

    def row_sum(k, pieces):
        high, low = halves(jnp.concatenate(pieces, axis=0))
        band = row_band[k]
        return jnp.dot(band, high, preferred_element_type=F32) + jnp.dot(band, low, preferred_element_type=F32)

    def tile_rows(t, slot, dst, at):
        same_copy(t, slot).wait_recv()

        @pl.when(inside)
        def _():
            other_copy(t, slot).wait_recv()

        for k in range(MOMENTS):
            dst[at, k] = row_sum(k, [part[t, slot, 0, k], part[t, slot, 1, k], same_got[t, k], other_got[t, k]])

    def give_back(t):
        tile_rows(t, OTH, to_direct, t)
        row_copy(t).start()

    def edge_sums(e, slot):
        t = edge_tile[e]
        theirs = OWN + OTH - slot
        edge_same_copy(e, theirs).wait_recv()

        @pl.when(inside)
        def _():
            edge_other_copy(e, theirs).wait_recv()

        i = theirs - 2
        return [
            row_sum(k, [part[t, slot, 0, k], part[t, slot, 1, k], edge_same[e, i, k], edge_other[e, i, k]])
            for k in range(MOMENTS)
        ]

    def edge_give(e):
        sums = edge_sums(e, OTH)
        for k in range(MOMENTS):
            to_direct[edge_tile[e], k] = sums[k]
        edge_row_copy(e).start()

    def edge_take(e):
        sums = edge_sums(e, OWN)
        edge_row_copy(e).wait_recv()
        for k in range(MOMENTS):
            rows[edge_tile[e] + 1, k] = sums[k] + from_rows[e, k]

    def finish(t, scales):
        start = pl.multiple_of(t * LANES, LANES)
        for k in range(MOMENTS):
            wide = jnp.concatenate([rows[t, k], rows[t + 1, k], rows[t + 2, k]], axis=1)
            high, low = halves(wide)
            band = col_band[k]
            total = jnp.dot(high, band, preferred_element_type=F32) + jnp.dot(low, band, preferred_element_type=F32)
            out[k, :, pl.ds(start, LANES)] = (total.reshape(8, 8, LANES) * scales[k][None]).reshape(64, LANES)

    barrier = pltpu.get_barrier_semaphore()

    def call(semaphore, where):
        pl.semaphore_signal(semaphore, inc=1, device_id=where, device_id_type=MESH)

    @pl.when(caller)
    def _():
        for friend in (to_core, to_partner, to_wrap):
            call(barrier, friend)

    @pl.when(callee)
    def _():
        call(barrier, to_far_core)

    @pl.when(jnp.logical_and(callee, inside))
    def _():
        call(barrier, to_wrap_other)

    order = []
    for i in range(max(inner, 2)):
        if i < inner:
            order.append(("away", i, away(i)))
        if i < 2:
            order.append(("edge", i, edge_tile[i]))
        if i < inner:
            order.append(("home", i, home(i)))
    ahead = 3
    for _, _, t in order[:ahead]:
        fetch(t)

    weight_sum = F32(0)
    for c in range(chans):
        weight = weights[c].astype(F32)
        weight_sum = weight_sum + weight
        offset = offsets[c]
        value = weight
        for k in range(MOMENTS):
            coef[k * chans + c] = value
            value = value * offset
    w_mine[...] = jnp.full((8, LANES), weight_sum, F32)

    near = lax.broadcasted_iota(jnp.int32, (64, LANES), 0)
    lane = lax.broadcasted_iota(jnp.int32, (64, LANES), 1)
    same_shift = jnp.where(odd == 1, -96, 0)
    other_shift = jnp.where(at_edge, 1000, jnp.where(odd == 1, -32, -128))
    place = lane + jnp.where(lane < 64, 0, jnp.where(lane < 96, same_shift, other_shift))
    row_gap = jnp.abs(place - near)
    for k in range(MOMENTS):
        row_band[k] = jnp.where(row_gap <= reach[k], 1.0, 0.0).astype(BF16)

    @pl.when(callee)
    def _():
        pl.semaphore_wait(barrier, 4)
        for friend in (to_core, to_partner, to_wrap):
            call(ready, friend)

    last = inner - 1
    long = inner >= 3

    def joined(kind, i, t):
        join(t)
        if kind == "edge":
            edge_same_copy(i, OWN).start()
            if i == 0:
                edge_same_copy(i, OTH).start()
        elif i == 0 or (i < last and not (long and i == 1 and kind == "away")):
            raw_copy(t, OWN if kind == "away" else OTH).start()

    def edge_others(slot):
        @pl.when(inside)
        def _():
            for e in range(2):
                edge_other_copy(e, slot).start()

    def meet():
        @pl.when(jnp.logical_and(caller, inside))
        def _():
            pl.semaphore_wait(barrier, 1)
            call(other_ready, to_wrap_other)

    def first_pair():
        @pl.when(jnp.logical_and(callee, inside))
        def _():
            pl.semaphore_wait(other_ready, 1)

        edge_others(OWN)
        complete(away(0), OTH)
        if long:
            raw_copy(away(1), OWN).start()
        edge_others(OTH)

    for i, (kind, at, t) in enumerate(order):
        moments(t, 0)
        if i == 0:

            @pl.when(caller)
            def _():
                pl.semaphore_wait(ready, 3)

            weight_copy(0).start()
        core_copy(t).start()
        if i + ahead < len(order):
            fetch(order[i + ahead][2])
        if i > 0:
            joined(*order[i - 1])
        moments(t, 2)
        if i == 1:
            weight_copy(0).wait_recv()
            w_pair[...] = w_mine[...] + w_got[0]
        if i == 2:
            weight_copy(1).start()
            meet()
        if i == 5 and long:
            first_pair()
        if i == 2 + inner:
            col_gap = jnp.abs(
                lax.broadcasted_iota(jnp.int32, (3 * LANES, LANES), 0) - LANES
                - lax.broadcasted_iota(jnp.int32, (3 * LANES, LANES), 1)
            )
            for k in range(MOMENTS):
                col_band[k] = jnp.where(col_gap <= reach[k], 1.0, 0.0).astype(BF16)
    joined(*order[-1])

    @pl.when(at_edge)
    def _():
        other_got[...] = jnp.zeros_like(other_got)
        edge_other[...] = jnp.zeros_like(edge_other)

    @pl.when(chan == 0)
    def _():
        rows[0] = jnp.zeros((MOMENTS, 64, LANES), F32)

    @pl.when(chan == 3)
    def _():
        rows[tiles + 1] = jnp.zeros((MOMENTS, 64, LANES), F32)

    if not long:
        first_pair()
    complete(home(0), OWN)
    if last > 0:
        raw_copy(home(last), OTH).start()
        raw_copy(away(last), OWN).start()
    for i in range(1, last):
        complete(away(i), OTH)
        complete(home(i), OWN)
    for e in range(2):
        edge_give(e)

    def rows_pair(i):
        give_back(away(i))
        tile_rows(home(i), OWN, rows, home(i) + 1)

    if last > 0:
        rows_pair(0)
        complete(home(last), OWN)
    edge_same_copy(1, OTH).start()
    if last > 0:
        complete(away(last), OTH)
    for i in range(1, last):
        rows_pair(i)
    give_back(away(last))
    for e in range(2):
        edge_take(e)

    @pl.when(chan > 0)
    def _():
        pack(1, 0, 0)
        left_edge().start()

    @pl.when(chan < 3)
    def _():
        pack(tiles, 1, 96)
        right_edge().start()

    tile_rows(home(last), OWN, rows, home(last) + 1)
    weight_copy(1).wait_recv()
    total = w_pair[...] + w_got[1]
    scales = [1.0 / (total * (2 * reach[k] + 1).astype(F32)) for k in range(MOMENTS)]

    @pl.when(chan < 3)
    def _():
        left_edge().wait_recv()
        unpack(tiles + 1, 1, 0)

    @pl.when(chan > 0)
    def _():
        right_edge().wait_recv()
        unpack(0, 0, 96)

    out_step = 1 - 2 * odd

    def last_steps(i, carry):
        finish(home(i) + out_step, scales)
        row_copy(away(i)).wait_recv()
        finish(away(i) - out_step, scales)
        return carry

    lax.fori_loop(0, inner, last_steps, 0)
    finish(home(inner - 1), scales)
    finish(away(inner - 1), scales)

    def sent(buffer, send):
        pltpu.make_async_copy(buffer, buffer, send).wait()

    middle = pl.ds(1, tiles - 2)
    sent(got, core_send)
    sent(raw_got.at[middle], raw_send)
    sent(same_got.at[middle], same_send)
    sent(edge_same, es_send)
    sent(rows.at[pl.ds(0, inner + 2)], row_send)

    @pl.when(inside)
    def _():
        sent(other_got.at[middle], other_send)
        sent(edge_other, eo_send)

    for i in range(2):
        weight_copy(i).wait_send()

    @pl.when(chan > 0)
    def _():
        left_edge().wait_send()

    @pl.when(chan < 3)
    def _():
        right_edge().wait_send()


def solution(mesh):
    slabs = mesh.shape["slab"]

    def body(beam, weights, offsets, reach):
        chans, height, width = beam.shape
        tiles = width // (4 * LANES)
        halo = (MOMENTS, 32, LANES)
        full = (MOMENTS, 64, LANES)
        dma = pltpu.SemaphoreType.DMA
        smem = pl.BlockSpec(memory_space=pltpu.SMEM)
        return pl.pallas_call(
            functools.partial(kernel, slabs, tiles, chans),
            out_shape=pltpu.VMEM((MOMENTS, height, width // 4), F32),
            in_specs=[pl.BlockSpec(memory_space=pl.ANY), smem, smem, smem],
            out_specs=pl.BlockSpec(memory_space=pltpu.VMEM),
            scratch_shapes=[
                pltpu.VMEM((tiles, 4, chans, 64, LANES), F32),
                pltpu.VMEM((tiles, 4, 2, *halo), F32),
                pltpu.VMEM((tiles, 2, 2, *halo), F32),
                pltpu.VMEM((tiles, 2, *halo), F32),
                pltpu.VMEM((tiles, *halo), F32),
                pltpu.VMEM((tiles, *halo), F32),
                pltpu.VMEM((2, 2, *halo), F32),
                pltpu.VMEM((2, 2, *halo), F32),
                pltpu.VMEM((tiles, *full), F32),
                pltpu.VMEM((2, *full), F32),
                pltpu.VMEM((tiles + 2, *full), F32),
                pltpu.VMEM((MOMENTS, 64, LANES), BF16),
                pltpu.VMEM((MOMENTS, 3 * LANES, LANES), BF16),
                pltpu.SMEM((MOMENTS * chans,), F32),
                pltpu.VMEM((8, LANES), F32),
                pltpu.VMEM((8, LANES), F32),
                pltpu.VMEM((2, 8, LANES), F32),
                pltpu.VMEM((2, MOMENTS, 16, LANES), F32),
                pltpu.VMEM((2, MOMENTS, 16, LANES), F32),
                dma((tiles, 2)),
                dma, dma((tiles,)),
                dma, dma((tiles,)),
                dma, dma((tiles,)),
                dma, dma((tiles,)),
                dma, dma((2, 2)),
                dma, dma((2, 2)),
                dma, dma((tiles,)),
                dma((2,)), dma((2,)),
                dma((2,)), dma((2,)),
                pltpu.SemaphoreType.REGULAR, pltpu.SemaphoreType.REGULAR,
            ],
            compiler_params=pltpu.CompilerParams(
                collective_id=0, has_side_effects=True, vmem_limit_bytes=60 * 1024 * 1024
            ),
        )(beam, weights, offsets, reach)

    placed = (P("chan", "slab", None), P("chan"), P("chan"), P())
    return jax.shard_map(
        body, mesh=mesh, in_specs=placed, out_specs=P(None, "slab", "chan"), check_vma=False
    )
```

```python
import functools

import jax
import jax.numpy as jnp
from jax import lax
from jax.experimental import pallas as pl
from jax.experimental.pallas import tpu as pltpu
from jax.sharding import PartitionSpec as P

MESH = pl.DeviceIdType.MESH
MOMENTS = 5
HW = 32
LANES = 128
F32 = jnp.float32
BF16 = jnp.bfloat16


def halves(value):
    high = value.astype(BF16)
    low = (value - high.astype(F32)).astype(BF16)
    return high, low


def kernel(
    slabs, tiles, chans,
    beam, weights, offsets, reach, out,
    pix, part, got, raw_got, same_got, other_got, edge_same, edge_other, to_direct, from_rows,
    rows, row_band, col_band, coef, w_mine, w_pair, w_got, edge_mine, edge_got,
    pix_sem, core_send, core_recv, raw_send, raw_recv, same_send, same_recv, other_send, other_recv,
    es_send, es_recv, eo_send, eo_recv, row_send, row_recv,
    edge_send, edge_recv, w_send, w_recv, ready, other_ready,
):
    chan = lax.axis_index("chan")
    slab = lax.axis_index("slab")
    odd = slab % 2
    partner = (chan + 2) % 4
    other_core = chan + 1 - 2 * (chan % 2)
    far_core = 3 - chan
    same_slab = slab + 1 - 2 * odd
    other_slab = (slab + slabs - 1 + 2 * odd) % slabs
    half_same = 1 - odd
    half_other = odd
    to_core = (other_core, slab)
    to_partner = (partner, slab)
    to_far_core = (far_core, slab)
    to_wrap = (partner, same_slab)
    to_wrap_other = (partner, other_slab)
    caller = jnp.logical_or(chan == 0, chan == 3)
    callee = jnp.logical_not(caller)
    at_edge = jnp.logical_or(slab == 0, slab == slabs - 1)
    inside = jnp.logical_not(at_edge)

    inner = (tiles - 2) // 2
    OWN, OTH = 2, 3

    def away(i):
        return (1 + i) * (1 - odd) + (tiles - 2 - i) * odd

    def home(i):
        return (1 + i) * odd + (tiles - 2 - i) * (1 - odd)

    edge_tile = (0, tiles - 1)

    def pixels(t, slot):
        quarter = (other_core, far_core, chan, partner)[slot]
        start = pl.multiple_of((quarter * tiles + t) * LANES, LANES)
        return pltpu.make_async_copy(beam.at[:, :, pl.ds(start, LANES)], pix.at[t, slot], pix_sem.at[t, slot // 2])

    def pixels_wait(t, pair):
        two = pix.at[t, pl.ds(2 * pair, 2)]
        pltpu.make_async_copy(two, two, pix_sem.at[t, pair]).wait()

    def remote(src, dst, send, recv, where):
        return pltpu.make_async_remote_copy(
            src_ref=src, dst_ref=dst, send_sem=send, recv_sem=recv, device_id=where, device_id_type=MESH
        )

    def core_copy(t):
        return remote(part.at[t, pl.ds(0, 2)], got.at[t], core_send, core_recv.at[t], to_core)

    def raw_copy(t, slot):
        return remote(part.at[t, slot], raw_got.at[t], raw_send, raw_recv.at[t], to_partner)

    def same_copy(t, slot):
        return remote(part.at[t, slot, half_same], same_got.at[t], same_send, same_recv.at[t], to_wrap)

    def other_copy(t, slot):
        return remote(part.at[t, slot, half_other], other_got.at[t], other_send, other_recv.at[t], to_wrap_other)

    def edge_same_copy(e, slot):
        src = part.at[edge_tile[e], slot, half_same]
        return remote(src, edge_same.at[e, slot - 2], es_send, es_recv.at[e, slot - 2], to_wrap)

    def edge_other_copy(e, slot):
        src = part.at[edge_tile[e], slot, half_other]
        return remote(src, edge_other.at[e, slot - 2], eo_send, eo_recv.at[e, slot - 2], to_wrap_other)

    def edge_row_copy(e):
        t = edge_tile[e]
        return remote(to_direct.at[t], from_rows.at[e], row_send, row_recv.at[t], to_partner)

    def row_copy(t):
        return remote(to_direct.at[t], rows.at[t + 1], row_send, row_recv.at[t], to_partner)

    def left_edge():
        return remote(edge_mine.at[0], edge_got.at[1], edge_send.at[0], edge_recv.at[1], ((chan + 3) % 4, slab))

    def right_edge():
        return remote(edge_mine.at[1], edge_got.at[0], edge_send.at[1], edge_recv.at[0], ((chan + 1) % 4, slab))

    def weight_copy(i):
        return remote((w_mine, w_pair)[i], w_got.at[i], w_send.at[i], w_recv.at[i], (to_core, to_partner)[i])

    def fetch(t):
        for slot in range(4):
            pixels(t, slot).start()

    def moments(t, first):
        pixels_wait(t, first // 2)

        def block(index, carry):
            slot = first + index // 2
            half = index % 2
            start = pl.multiple_of(half * 32, 32)
            totals = [None] * MOMENTS
            for c in range(chans):
                x = pix[t, slot, c, pl.ds(start, 32), :]
                for k in range(MOMENTS):
                    term = coef[k * chans + c] * x
                    totals[k] = term if c == 0 else totals[k] + term
            for k in range(MOMENTS):
                part[t, slot, half, k] = totals[k]
            return carry

        lax.fori_loop(0, 4, block, 0)

    def join(t):
        core_copy(t).wait_recv()

        def add(index, carry):
            side = index // 2
            half = index % 2
            for k in range(MOMENTS):
                part[t, 2 + side, half, k] = part[t, 2 + side, half, k] + got[t, side, half, k]
            return carry

        lax.fori_loop(0, 4, add, 0)

    def complete(t, slot):
        raw_copy(t, slot).wait_recv()
        for half in range(2):
            for k in range(MOMENTS):
                part[t, slot, half, k] = part[t, slot, half, k] + raw_got[t, half, k]

        @pl.when(inside)
        def _():
            other_copy(t, slot).start()

        same_copy(t, slot).start()

    lane_of = lax.broadcasted_iota(jnp.int32, (16, LANES), 1)

    def pack(index, side, first):
        for k in range(MOMENTS):
            packed = jnp.zeros((16, LANES), F32)
            for group in range(4):
                piece = rows[index, k, pl.ds(16 * group, 16), :]
                shift = (32 * group - first) % LANES
                piece = piece if shift == 0 else pltpu.roll(piece, shift, 1)
                packed = jnp.where(lane_of // 32 == group, piece, packed)
            edge_mine[side, k] = packed

    def unpack(index, side, first):
        for k in range(MOMENTS):
            packed = edge_got[side, k]
            for group in range(4):
                shift = (first - 32 * group) % LANES
                piece = packed if shift == 0 else pltpu.roll(packed, shift, 1)
                rows[index, k, pl.ds(16 * group, 16), :] = jnp.where(lane_of // 32 == first // 32, piece, 0.0)

    def row_sum(k, pieces):
        high, low = halves(jnp.concatenate(pieces, axis=0))
        band = row_band[k]
        return jnp.dot(band, high, preferred_element_type=F32) + jnp.dot(band, low, preferred_element_type=F32)

    def tile_rows(t, slot, dst, at):
        same_copy(t, slot).wait_recv()

        @pl.when(inside)
        def _():
            other_copy(t, slot).wait_recv()

        for k in range(MOMENTS):
            dst[at, k] = row_sum(k, [part[t, slot, 0, k], part[t, slot, 1, k], same_got[t, k], other_got[t, k]])

    def give_back(t):
        tile_rows(t, OTH, to_direct, t)
        row_copy(t).start()

    def edge_sums(e, slot):
        t = edge_tile[e]
        theirs = OWN + OTH - slot
        edge_same_copy(e, theirs).wait_recv()

        @pl.when(inside)
        def _():
            edge_other_copy(e, theirs).wait_recv()

        i = theirs - 2
        return [
            row_sum(k, [part[t, slot, 0, k], part[t, slot, 1, k], edge_same[e, i, k], edge_other[e, i, k]])
            for k in range(MOMENTS)
        ]

    def edge_give(e):
        sums = edge_sums(e, OTH)
        for k in range(MOMENTS):
            to_direct[edge_tile[e], k] = sums[k]
        edge_row_copy(e).start()

    def edge_take(e):
        sums = edge_sums(e, OWN)
        edge_row_copy(e).wait_recv()
        for k in range(MOMENTS):
            rows[edge_tile[e] + 1, k] = sums[k] + from_rows[e, k]

    def finish(t, scales):
        start = pl.multiple_of(t * LANES, LANES)
        for k in range(MOMENTS):
            wide = jnp.concatenate([rows[t, k], rows[t + 1, k], rows[t + 2, k]], axis=1)
            high, low = halves(wide)
            band = col_band[k]
            total = jnp.dot(high, band, preferred_element_type=F32) + jnp.dot(low, band, preferred_element_type=F32)
            out[k, :, pl.ds(start, LANES)] = (total.reshape(8, 8, LANES) * scales[k][None]).reshape(64, LANES)

    barrier = pltpu.get_barrier_semaphore()

    def call(semaphore, where):
        pl.semaphore_signal(semaphore, inc=1, device_id=where, device_id_type=MESH)

    @pl.when(caller)
    def _():
        for friend in (to_core, to_partner, to_wrap):
            call(barrier, friend)

    @pl.when(callee)
    def _():
        call(barrier, to_far_core)

    @pl.when(jnp.logical_and(callee, inside))
    def _():
        call(barrier, to_wrap_other)

    order = []
    for i in range(max(inner, 2)):
        if i < inner:
            order.append(("away", i, away(i)))
        if i < 2:
            order.append(("edge", i, edge_tile[i]))
        if i < inner:
            order.append(("home", i, home(i)))
    ahead = 3
    for _, _, t in order[:ahead]:
        fetch(t)

    weight_sum = F32(0)
    for c in range(chans):
        weight = weights[c].astype(F32)
        weight_sum = weight_sum + weight
        offset = offsets[c]
        value = weight
        for k in range(MOMENTS):
            coef[k * chans + c] = value
            value = value * offset
    w_mine[...] = jnp.full((8, LANES), weight_sum, F32)

    near = lax.broadcasted_iota(jnp.int32, (64, LANES), 0)
    lane = lax.broadcasted_iota(jnp.int32, (64, LANES), 1)
    same_shift = jnp.where(odd == 1, -96, 0)
    other_shift = jnp.where(at_edge, 1000, jnp.where(odd == 1, -32, -128))
    place = lane + jnp.where(lane < 64, 0, jnp.where(lane < 96, same_shift, other_shift))
    row_gap = jnp.abs(place - near)
    for k in range(MOMENTS):
        row_band[k] = jnp.where(row_gap <= reach[k], 1.0, 0.0).astype(BF16)

    @pl.when(callee)
    def _():
        pl.semaphore_wait(barrier, 4)
        for friend in (to_core, to_partner, to_wrap):
            call(ready, friend)

    last = inner - 1
    long = inner >= 3

    def joined(kind, i, t):
        join(t)
        if kind == "edge":
            edge_same_copy(i, OWN).start()
            edge_same_copy(i, OTH).start()
        elif i == 0 or (i < last and not (long and i == 1 and kind == "away")):
            raw_copy(t, OWN if kind == "away" else OTH).start()

    def edge_others(slot):
        @pl.when(inside)
        def _():
            for e in range(2):
                edge_other_copy(e, slot).start()

    def meet():
        @pl.when(jnp.logical_and(caller, inside))
        def _():
            pl.semaphore_wait(barrier, 1)
            call(other_ready, to_wrap_other)

    def first_pair():
        @pl.when(jnp.logical_and(callee, inside))
        def _():
            pl.semaphore_wait(other_ready, 1)

        edge_others(OWN)
        complete(away(0), OTH)
        if long:
            raw_copy(away(1), OWN).start()
        edge_others(OTH)

    for i, (kind, at, t) in enumerate(order):
        moments(t, 0)
        if i == 0:

            @pl.when(caller)
            def _():
                pl.semaphore_wait(ready, 3)

            weight_copy(0).start()
        core_copy(t).start()
        if i + ahead < len(order):
            fetch(order[i + ahead][2])
        if i > 0:
            joined(*order[i - 1])
        moments(t, 2)
        if i == 1:
            weight_copy(0).wait_recv()
            w_pair[...] = w_mine[...] + w_got[0]
        if i == 2:
            weight_copy(1).start()
            meet()
        if i == 5 and long:
            first_pair()
        if i == 2 + inner:
            col_gap = jnp.abs(
                lax.broadcasted_iota(jnp.int32, (3 * LANES, LANES), 0) - LANES
                - lax.broadcasted_iota(jnp.int32, (3 * LANES, LANES), 1)
            )
            for k in range(MOMENTS):
                col_band[k] = jnp.where(col_gap <= reach[k], 1.0, 0.0).astype(BF16)
    joined(*order[-1])

    @pl.when(at_edge)
    def _():
        other_got[...] = jnp.zeros_like(other_got)
        edge_other[...] = jnp.zeros_like(edge_other)

    @pl.when(chan == 0)
    def _():
        rows[0] = jnp.zeros((MOMENTS, 64, LANES), F32)

    @pl.when(chan == 3)
    def _():
        rows[tiles + 1] = jnp.zeros((MOMENTS, 64, LANES), F32)

    if not long:
        first_pair()
    complete(home(0), OWN)
    if last > 0:
        raw_copy(home(last), OTH).start()
        raw_copy(away(last), OWN).start()
    for i in range(1, last):
        complete(away(i), OTH)
        complete(home(i), OWN)
    for e in range(2):
        edge_give(e)

    def rows_pair(i):
        give_back(away(i))
        tile_rows(home(i), OWN, rows, home(i) + 1)

    if last > 0:
        rows_pair(0)
        complete(home(last), OWN)
    if last > 0:
        complete(away(last), OTH)
    for i in range(1, last):
        rows_pair(i)
    if last == 0:
        give_back(away(last))
    for e in range(2):
        edge_take(e)

    @pl.when(chan > 0)
    def _():
        pack(1, 0, 0)
        left_edge().start()

    @pl.when(chan < 3)
    def _():
        pack(tiles, 1, 96)
        right_edge().start()

    if last > 0:
        give_back(away(last))

    weight_copy(1).wait_recv()
    total = w_pair[...] + w_got[1]
    scales = [1.0 / (total * (2 * reach[k] + 1).astype(F32)) for k in range(MOMENTS)]
    out_step = 1 - 2 * odd

    def home_step(i, carry):
        finish(home(i) + out_step, scales)
        return carry

    def away_step(i, carry):
        row_copy(away(i)).wait_recv()
        finish(away(i) - out_step, scales)
        return carry

    lax.fori_loop(1, last, home_step, 0)
    if last > 0:
        row_copy(away(0)).wait_recv()
    lax.fori_loop(1, last, away_step, 0)
    tile_rows(home(last), OWN, rows, home(last) + 1)
    lax.fori_loop(max(last, 1), last + 1, home_step, 0)
    if last > 0:
        lax.fori_loop(last, last + 1, away_step, 0)
    else:
        row_copy(away(0)).wait_recv()
    finish(home(last), scales)
    finish(away(last), scales)

    @pl.when(chan > 0)
    def _():
        right_edge().wait_recv()
        unpack(0, 0, 96)

    @pl.when(chan < 3)
    def _():
        left_edge().wait_recv()
        unpack(tiles + 1, 1, 0)

    lax.fori_loop(0, 2, lambda e, carry: (finish(e * (tiles - 1), scales), carry)[1], 0)

    def sent(buffer, send):
        pltpu.make_async_copy(buffer, buffer, send).wait()

    middle = pl.ds(1, tiles - 2)
    sent(got, core_send)
    sent(raw_got.at[middle], raw_send)
    sent(same_got.at[middle], same_send)
    sent(edge_same, es_send)
    sent(rows.at[pl.ds(0, inner + 2)], row_send)

    @pl.when(inside)
    def _():
        sent(other_got.at[middle], other_send)
        sent(edge_other, eo_send)

    for i in range(2):
        weight_copy(i).wait_send()

    @pl.when(chan > 0)
    def _():
        left_edge().wait_send()

    @pl.when(chan < 3)
    def _():
        right_edge().wait_send()


def solution(mesh):
    slabs = mesh.shape["slab"]

    def body(beam, weights, offsets, reach):
        chans, height, width = beam.shape
        tiles = width // (4 * LANES)
        halo = (MOMENTS, 32, LANES)
        full = (MOMENTS, 64, LANES)
        dma = pltpu.SemaphoreType.DMA
        smem = pl.BlockSpec(memory_space=pltpu.SMEM)
        return pl.pallas_call(
            functools.partial(kernel, slabs, tiles, chans),
            out_shape=pltpu.VMEM((MOMENTS, height, width // 4), F32),
            in_specs=[pl.BlockSpec(memory_space=pl.ANY), smem, smem, smem],
            out_specs=pl.BlockSpec(memory_space=pltpu.VMEM),
            scratch_shapes=[
                pltpu.VMEM((tiles, 4, chans, 64, LANES), F32),
                pltpu.VMEM((tiles, 4, 2, *halo), F32),
                pltpu.VMEM((tiles, 2, 2, *halo), F32),
                pltpu.VMEM((tiles, 2, *halo), F32),
                pltpu.VMEM((tiles, *halo), F32),
                pltpu.VMEM((tiles, *halo), F32),
                pltpu.VMEM((2, 2, *halo), F32),
                pltpu.VMEM((2, 2, *halo), F32),
                pltpu.VMEM((tiles, *full), F32),
                pltpu.VMEM((2, *full), F32),
                pltpu.VMEM((tiles + 2, *full), F32),
                pltpu.VMEM((MOMENTS, 64, LANES), BF16),
                pltpu.VMEM((MOMENTS, 3 * LANES, LANES), BF16),
                pltpu.SMEM((MOMENTS * chans,), F32),
                pltpu.VMEM((8, LANES), F32),
                pltpu.VMEM((8, LANES), F32),
                pltpu.VMEM((2, 8, LANES), F32),
                pltpu.VMEM((2, MOMENTS, 16, LANES), F32),
                pltpu.VMEM((2, MOMENTS, 16, LANES), F32),
                dma((tiles, 2)),
                dma, dma((tiles,)),
                dma, dma((tiles,)),
                dma, dma((tiles,)),
                dma, dma((tiles,)),
                dma, dma((2, 2)),
                dma, dma((2, 2)),
                dma, dma((tiles,)),
                dma((2,)), dma((2,)),
                dma((2,)), dma((2,)),
                pltpu.SemaphoreType.REGULAR, pltpu.SemaphoreType.REGULAR,
            ],
            compiler_params=pltpu.CompilerParams(
                collective_id=0, has_side_effects=True, vmem_limit_bytes=60 * 1024 * 1024
            ),
        )(beam, weights, offsets, reach)

    placed = (P("chan", "slab", None), P("chan"), P("chan"), P())
    return jax.shard_map(
        body, mesh=mesh, in_specs=placed, out_specs=P(None, "slab", "chan"), check_vma=False
    )
```
